32 devices in a mesh: fsdp: 4 (over z), ctx: 2 (over y), tp: 4 (over x, core).
Axes of the slice: x: 2, y: 2, z: 4, core: 2. Of those that a mesh axis runs over, the one named last changes fastest.
Arguments:
- layer_input: bfloat16 [8192, 768], P(('fsdp', 'ctx')), may hold values from -6 to 6
- segments: int32 [8192], P('fsdp'), may hold values from 0 to 7, as said below
- positions: int32 [8192], P(('fsdp', 'ctx')), may hold values from 0 to 1535, as said below
- ln1_gain: float32 [768], replicated, may hold values from 0.1 to 1.9
- ln1_bias: float32 [768], replicated, may hold values from -3 to 3
- ln2_gain: float32 [768], replicated, may hold values from 0.1 to 1.9
- ln2_bias: float32 [768], replicated, may hold values from -3 to 3
- w_qkv: bfloat16 [768, 3, 768], P('fsdp', None, 'tp'), as said below
- b_qkv: float32 [3, 768], P(None, 'tp'), may hold values from -3 to 3
- w_out: bfloat16 [768, 768], P('tp', 'fsdp'), may hold values from -1.75 to 1.75
- b_out: float32 [768], replicated, may hold values from -3 to 3
- w_fc1: bfloat16 [768, 3072], P('fsdp', 'tp'), may hold values from -0.21875 to 0.21875
- b_fc1: float32 [3072], P('tp'), may hold values from -3 to 3
- w_fc2: bfloat16 [3072, 768], P('tp', 'fsdp'), may hold values from -0.109375 to 0.109375
- b_fc2: float32 [768], replicated, may hold values from -3 to 3
- out_grad: float32 [8192, 768], P(('fsdp', 'ctx')), may hold values from -6 to 6
Outputs:
- block_out: float32 [8192, 768], P(('fsdp', 'ctx'))
- input_grad: float32 [8192, 768], P(('fsdp', 'ctx'))
- g_ln1_gain: float32 [768], replicated
- g_ln1_bias: float32 [768], replicated
- g_ln2_gain: float32 [768], replicated
- g_ln2_bias: float32 [768], replicated
- g_w_qkv: float32 [768, 3, 768], P('fsdp', None, 'tp')
- g_b_qkv: float32 [3, 768], P(None, 'tp')
- g_w_out: float32 [768, 768], P('tp', 'fsdp')
- g_b_out: float32 [768], replicated
- g_w_fc1: float32 [768, 3072], P('fsdp', 'tp')
- g_b_fc1: float32 [3072], P('tp')
- g_w_fc2: float32 [3072, 768], P('tp', 'fsdp')
- g_b_fc2: float32 [768], replicated
The draws below stay inside these ranges and needn't reach their ends.
Inputs may be any that keep to these rules, and one draw needn't show every extreme that they name: `segments`: within each sequence of 2048 tokens the numbers never fall, start at 0, and every value up to 7 appears; document 0 covers exactly the first 1536 tokens of each sequence. `positions`: the offset of a token from the first token of its document. `w_qkv`: entries of order 768 ** -0.5, up to a factor of a few.
All inputs are finite; a program needn't handle non-finite values.
Results may differ from the reference program's by a relative error of at most 0.012.
Values may be sent and summed in bfloat16 or wider, within the bound.
A program may use at most 128 MiB of HBM per device.

```python
import math
import jax
import jax.numpy as jnp
from jax import lax

D = 768
H = 12
HD = 64
FF = 3072
ROT = 16
DOCS = 8
LENGTH = 2048
SEQS = 4
TOKENS = 8192


def doc_layout(key):
    base_key = jax.random.fold_in(key, 71)
    seq_keys = jax.random.split(base_key, SEQS)
    long_len = 3 * (LENGTH // 4)
    tail_len = LENGTH - long_len

    def one_sequence(seq_key):
        inner = (jax.random.permutation(seq_key, tail_len - 1)[:DOCS - 2] + 1 + long_len).astype(jnp.int32)
        cuts = jnp.concatenate([inner, jnp.full((1,), long_len, jnp.int32)]).astype(jnp.int32)
        index_all = jnp.arange(LENGTH, dtype=jnp.int32)
        passed = cuts[None, :] <= index_all[:, None]
        seg_ids = jnp.sum(passed.astype(jnp.int32), axis=1)
        begins = jnp.max(jnp.where(passed, cuts[None, :], 0), axis=1)
        return (seg_ids.astype(jnp.int32), (index_all - begins).astype(jnp.int32))
    seg_ids, offsets = jax.vmap(one_sequence)(seq_keys)
    return (seg_ids.reshape(-1), offsets.reshape(-1))


def draw_segments(key, part):
    return doc_layout(key)[0]


def draw_positions(key, part):
    return doc_layout(key)[1]


def draw_w_qkv(key, part):
    base = jax.random.normal(jax.random.fold_in(key, 5), (D, 3, H * HD), jnp.float32) * D ** (-0.5)
    return base.astype(jnp.bfloat16)


def steps_of(stream_key, extent, cuts, low, high):
    level, own = 1.0, jax.random.fold_in(stream_key, 6)
    for position, shards_of in cuts:
        heights = jnp.exp(jax.random.uniform(jax.random.fold_in(own, position), (shards_of,), jnp.float32, low / len(cuts), high / len(cuts)))
        level = level * jnp.repeat(heights, extent[position] // shards_of).reshape([-1 if axis == position else 1 for axis in range(len(extent))])
    return level


def bell_draw(key, shape, spread, limit, shards=(), held_as=jnp.bfloat16):
    values = jax.random.normal(key, shape, jnp.float32) * spread
    if len(shards) > 0:
        values = steps_of(key, shape, shards, -0.22, 0.18) * values
    return jnp.clip(values, min=-limit, max=limit).astype(held_as)


def setup_inputs(seed: int = 0) -> dict:
    streams_of = jax.random.split(jax.random.key(seed), 17)
    return {
        "layer_input": bell_draw(streams_of[0], (TOKENS, D), 1.0, 6.0, ((0, 8),)),
        "segments": draw_segments(jax.random.fold_in(streams_of[16], 71), 0),
        "positions": draw_positions(jax.random.fold_in(streams_of[16], 71), 0),
        "ln1_gain": jnp.clip(1.0 + 0.18 * jax.random.normal(streams_of[3], (D,), jnp.float32), 0.1, 1.9),
        "ln1_bias": bell_draw(streams_of[4], (D,), 0.5, 3.0, (), jnp.float32),
        "ln2_gain": jnp.clip(1.0 + 0.18 * jax.random.normal(streams_of[5], (D,), jnp.float32), 0.1, 1.9),
        "ln2_bias": bell_draw(streams_of[6], (D,), 0.5, 3.0, (), jnp.float32),
        "w_qkv": draw_w_qkv(jax.random.fold_in(streams_of[16], 71), 0),
        "b_qkv": bell_draw(streams_of[8], (3, H * HD), 0.5, 3.0, ((1, 4),), jnp.float32),
        "w_out": bell_draw(streams_of[9], (H * HD, D), (H * HD // 64) ** -0.5, 1.75, ((0, 4), (1, 4))),
        "b_out": bell_draw(streams_of[10], (D,), 0.5, 3.0, (), jnp.float32),
        "w_fc1": bell_draw(streams_of[11], (D, FF), D ** -0.5, 0.21875, ((0, 4), (1, 4))),
        "b_fc1": bell_draw(streams_of[12], (FF,), 0.5, 3.0, ((0, 4),), jnp.float32),
        "w_fc2": bell_draw(streams_of[13], (FF, D), FF ** -0.5, 0.109375, ((0, 4), (1, 4))),
        "b_fc2": bell_draw(streams_of[14], (D,), 0.5, 3.0, (), jnp.float32),
        "out_grad": bell_draw(streams_of[15], (TOKENS, D), 1.0, 6.0, ((0, 8),), jnp.float32),
    }


NEG_FILL = -1e+30
NORM_EPS = 1e-05
INV_ROOT_TWO = 0.7071067811865476
INV_ROOT_TWO_PI = 0.3989422804014327

def to_half(values):
    return lax.optimization_barrier(values.astype(jnp.bfloat16)).astype(jnp.float32)

def layer_stats(inputs, gain, shift):
    centre = lax.optimization_barrier(jnp.mean(inputs, -1, keepdims=True))
    centred = inputs - centre
    inverse = lax.rsqrt(lax.optimization_barrier(jnp.mean(centred * centred, -1, keepdims=True)) + NORM_EPS)
    normed = centred * inverse
    return (normed, inverse, normed * gain + shift)

def layer_back(upstream, normed, inverse, gain):
    scaled = upstream * gain
    d_input = inverse * (scaled - lax.optimization_barrier(jnp.mean(scaled, -1, keepdims=True)) - normed * lax.optimization_barrier(jnp.mean(scaled * normed, -1, keepdims=True)))
    return (d_input, lax.optimization_barrier(jnp.sum(upstream * normed, 0)), lax.optimization_barrier(jnp.sum(upstream, 0)))

def rotary_tables(offsets, rot_dims):
    half_dims = rot_dims // 2
    freqs = 10000.0 ** (-(jnp.arange(half_dims, dtype=jnp.float32) * 2.0) / rot_dims)
    angles = offsets.astype(jnp.float32)[:, None] * freqs[None, :]
    angles = jnp.concatenate([angles, angles], -1)[:, None, :]
    return (jnp.cos(angles), jnp.sin(angles))

def rotate_fwd(tensor, cosine, sine, rot_dims):
    half_dims = rot_dims // 2
    part = tensor[..., :rot_dims]
    turned = jnp.concatenate([-part[..., half_dims:], part[..., :half_dims]], -1)
    return jnp.concatenate([part * cosine + turned * sine, tensor[..., rot_dims:]], -1)

def rotate_back(upstream, cosine, sine, rot_dims):
    half_dims = rot_dims // 2
    part = upstream[..., :rot_dims]
    scaled = part * sine
    turned = jnp.concatenate([scaled[..., half_dims:], -scaled[..., :half_dims]], -1)
    return jnp.concatenate([part * cosine + turned, upstream[..., rot_dims:]], -1)

def gelu_parts(pre_act):
    normal_cdf = 0.5 * (1.0 + lax.erf(pre_act * INV_ROOT_TWO))
    density = jnp.exp(-0.5 * pre_act * pre_act) * INV_ROOT_TWO_PI
    return (pre_act * normal_cdf, normal_cdf + pre_act * density)

def reference(layer_input, segments, positions, ln1_gain, ln1_bias, ln2_gain, ln2_bias, w_qkv, b_qkv, w_out, b_out, w_fc1, b_fc1, w_fc2, b_fc2, out_grad):
    head_span = H * HD
    score_scale = HD ** (-0.5)
    q_rows = math.gcd(LENGTH, 256)
    q_blocks = LENGTH // q_rows
    w_flat = w_qkv.reshape(D, 3 * head_span)
    key_index = jnp.arange(LENGTH, dtype=jnp.int32)

    def one_sequence(sums, item):
        seq_input, seq_segments, seq_positions, seq_grad = item
        inputs_f = seq_input.astype(jnp.float32)
        normed_one, inverse_one, affine_one = layer_stats(inputs_f, ln1_gain, ln1_bias)
        normed_two, inverse_two, affine_two = layer_stats(inputs_f, ln2_gain, ln2_bias)
        hidden_one = affine_one.astype(jnp.bfloat16)
        hidden_two = affine_two.astype(jnp.bfloat16)
        projected = jnp.dot(hidden_one, w_flat, preferred_element_type=jnp.float32).reshape(LENGTH, 3, head_span) + b_qkv
        cosine, sine = rotary_tables(seq_positions, ROT)
        query = rotate_fwd(projected[:, 0].reshape(LENGTH, H, HD), cosine, sine, ROT).astype(jnp.bfloat16)
        keys = rotate_fwd(projected[:, 1].reshape(LENGTH, H, HD), cosine, sine, ROT).astype(jnp.bfloat16)
        values = projected[:, 2].reshape(LENGTH, H, HD).astype(jnp.bfloat16)
        keys_f = keys.astype(jnp.float32)
        values_f = values.astype(jnp.float32)
        seg_blocks = seq_segments.reshape(q_blocks, q_rows)
        idx_blocks = key_index.reshape(q_blocks, q_rows)

        def allowed_of(q_seg, q_idx):
            return ((seq_segments[None, :] == q_seg[:, None]) & (key_index[None, :] <= q_idx[:, None]))[None]

        def attend(item_blk):
            q_blk, q_seg, q_idx = item_blk
            allowed = allowed_of(q_seg, q_idx)
            scores = jnp.einsum('qhd,khd->hqk', q_blk.astype(jnp.float32), keys_f) * score_scale
            scores = jnp.where(allowed, scores, NEG_FILL)
            row_top = lax.optimization_barrier(jnp.max(scores, -1))
            weights = jnp.where(allowed, jnp.exp(scores - row_top[..., None]), 0.0)
            row_total = lax.optimization_barrier(jnp.sum(weights, -1))
            mixed = jnp.einsum('hqk,khd->qhd', to_half(weights), values_f) / jnp.transpose(row_total)[:, :, None]
            return (mixed, row_top + jnp.log(row_total))
        context, log_total = lax.map(attend, (query.reshape(q_blocks, q_rows, H, HD), seg_blocks, idx_blocks))
        context_b = context.reshape(LENGTH, H, HD).astype(jnp.bfloat16)
        context_flat = context_b.reshape(LENGTH, head_span)
        attn_part = jnp.dot(context_flat, w_out, preferred_element_type=jnp.float32)
        pre_act = jnp.dot(hidden_two, w_fc1, preferred_element_type=jnp.float32) + b_fc1
        activated, slope = gelu_parts(pre_act)
        act_b = activated.astype(jnp.bfloat16)
        mlp_part = jnp.dot(act_b, w_fc2, preferred_element_type=jnp.float32)
        result = inputs_f + attn_part + mlp_part + b_out + b_fc2
        grad_b = seq_grad.astype(jnp.bfloat16)
        g_fc2 = jnp.dot(act_b.T, grad_b, preferred_element_type=jnp.float32)
        d_pre = jnp.dot(grad_b, w_fc2.T, preferred_element_type=jnp.float32) * slope
        d_pre_b = d_pre.astype(jnp.bfloat16)
        g_fc1 = jnp.dot(hidden_two.T, d_pre_b, preferred_element_type=jnp.float32)
        d_hidden_two = jnp.dot(d_pre_b, w_fc1.T, preferred_element_type=jnp.float32)
        g_wout = jnp.dot(context_flat.T, grad_b, preferred_element_type=jnp.float32)
        d_context = jnp.dot(grad_b, w_out.T, preferred_element_type=jnp.float32).astype(jnp.bfloat16).reshape(LENGTH, H, HD)
        delta = jnp.einsum('qhd,qhd->hq', d_context.astype(jnp.float32), context_b.astype(jnp.float32))
        delta_blocks = jnp.transpose(delta.reshape(H, q_blocks, q_rows), (1, 0, 2))

        def back(carry, item_blk):
            d_keys, d_values = carry
            q_blk, do_blk, lse_blk, delta_blk, q_seg, q_idx = item_blk
            allowed = allowed_of(q_seg, q_idx)
            q_f = q_blk.astype(jnp.float32)
            do_f = do_blk.astype(jnp.float32)
            scores = jnp.einsum('qhd,khd->hqk', q_f, keys_f) * score_scale
            prob = jnp.where(allowed, jnp.exp(scores - lse_blk[..., None]), 0.0)
            d_prob = jnp.einsum('qhd,khd->hqk', do_f, values_f)
            d_scores = to_half(prob * (d_prob - delta_blk[..., None]) * score_scale)
            d_query = jnp.einsum('hqk,khd->qhd', d_scores, keys_f)
            d_keys = d_keys + jnp.einsum('hqk,qhd->khd', d_scores, q_f)
            d_values = d_values + jnp.einsum('hqk,qhd->khd', to_half(prob), do_f)
            return ((d_keys, d_values), d_query)
        zeros_kv = jnp.zeros((LENGTH, H, HD), jnp.float32)
        (d_keys, d_values), d_query = lax.scan(back, (zeros_kv, zeros_kv), (query.reshape(q_blocks, q_rows, H, HD), d_context.reshape(q_blocks, q_rows, H, HD), log_total, delta_blocks, seg_blocks, idx_blocks))
        d_query = d_query.reshape(LENGTH, H, HD)
        d_projected = jnp.stack([rotate_back(d_query, cosine, sine, ROT).reshape(LENGTH, head_span), rotate_back(d_keys, cosine, sine, ROT).reshape(LENGTH, head_span), d_values.reshape(LENGTH, head_span)], 1)
        g_bqkv = lax.optimization_barrier(jnp.sum(d_projected, 0))
        d_proj_b = d_projected.astype(jnp.bfloat16).reshape(LENGTH, 3 * head_span)
        g_wqkv = jnp.dot(hidden_one.T, d_proj_b, preferred_element_type=jnp.float32)
        d_hidden_one = jnp.dot(d_proj_b, w_flat.T, preferred_element_type=jnp.float32)
        dx_one, g_gain_one, g_shift_one = layer_back(d_hidden_one, normed_one, inverse_one, ln1_gain)
        dx_two, g_gain_two, g_shift_two = layer_back(d_hidden_two, normed_two, inverse_two, ln2_gain)
        d_input = seq_grad + dx_one + dx_two
        terms = (g_gain_one, g_shift_one, g_gain_two, g_shift_two, g_wqkv, g_bqkv, g_wout, lax.optimization_barrier(jnp.sum(seq_grad, 0)), g_fc1, lax.optimization_barrier(jnp.sum(d_pre, 0)), g_fc2)
        return (jax.tree.map(jnp.add, sums, terms), (result, d_input))
    initial = (jnp.zeros((D,), jnp.float32), jnp.zeros((D,), jnp.float32), jnp.zeros((D,), jnp.float32), jnp.zeros((D,), jnp.float32), jnp.zeros((D, 3 * head_span), jnp.float32), jnp.zeros((3, head_span), jnp.float32), jnp.zeros((head_span, D), jnp.float32), jnp.zeros((D,), jnp.float32), jnp.zeros((D, FF), jnp.float32), jnp.zeros((FF,), jnp.float32), jnp.zeros((FF, D), jnp.float32))
    sums, (outputs, d_inputs) = lax.scan(one_sequence, initial, (layer_input.reshape(SEQS, LENGTH, D), segments.reshape(SEQS, LENGTH), positions.reshape(SEQS, LENGTH), out_grad.reshape(SEQS, LENGTH, D)))
    return (outputs.reshape(TOKENS, D), d_inputs.reshape(TOKENS, D), sums[0], sums[1], sums[2], sums[3], sums[4].reshape(D, 3, head_span), sums[5], sums[6], sums[7], sums[8], sums[9], sums[10], sums[7])
```

```python
import jax
import jax.numpy as jnp
from jax import lax
from jax.experimental import pallas as pl
from jax.experimental.pallas import tpu as pltpu
from jax.sharding import PartitionSpec as P

HD = 64
ROT = 16
HALF = ROT // 2
NEG_FILL = -1e30
NORM_EPS = 1e-05
INV_ROOT_TWO = 0.7071067811865476
INV_ROOT_TWO_PI = 0.3989422804014327
F32 = jnp.float32
BF16 = jnp.bfloat16
VMEM_BYTES = 67043328


def mm(a, b):
    return jnp.dot(a, b, preferred_element_type=F32)


def mm_nt(a, b):
    return lax.dot_general(a, b, (((1,), (1,)), ((), ())), preferred_element_type=F32)


def tile_rows(i, size):
    return pl.ds(pl.multiple_of(i * size, size), size)


class Dims:
    def __init__(self, mesh, tokens, width, span, hidden):
        self.nz, self.nc, self.nt = mesh.shape["fsdp"], mesh.shape["ctx"], mesh.shape["tp"]
        self.tok, self.width, self.span, self.hidden = tokens, width, span, hidden
        self.heads = span // HD
        self.blk = min(512, tokens)
        self.nb = tokens // self.blk
        self.nkb = self.nc * self.nb
        self.tail = (3 * self.nkb) // 4
        self.rows = width // self.nz
        self.half = self.rows // 2
        self.tile = min(256, tokens)
        self.nx = self.nt // 2
        self.keep = self.nc <= 2
        assert 4 * span == hidden and self.nt % 2 == 0 and self.nc % 2 == 0
        self.wide = max(width, hidden, 3 * span)
        nz, nc, nx = self.nz, self.nc, self.nx
        self.n_copies = (
            3 * 2 * (nz - 1)
            + 2 * (nc - 1)
            + 2 * (nx + 1)
            + 3 * (1 + (nz - 1) + (nc - 1))
            + (nz * nc - 1)
            + (self.nt - 1)
        )


class Net:
    def __init__(self, send, recv):
        self.send, self.recv, self.used, self.started = send, recv, 0, []

    def copy(self, src, dst, device):
        i = self.used
        self.used += 1
        return pltpu.make_async_remote_copy(
            src_ref=src,
            dst_ref=dst,
            send_sem=self.send.at[i],
            recv_sem=self.recv.at[i],
            device_id=device,
            device_id_type=pl.DeviceIdType.MESH,
        )


def layer_kernel(d, *refs):
    (x, og, pos, cosr, sinr, vec, bq, bf1, wa, wb, wc) = refs[:11]
    (out, ig, ga, gb_out, gc_out, sm_out) = refs[11:17]
    (
        WA, WB, WC, WT, h1, h2, tA, gb, gbT, mean_s, inv_s, act, dpre,
        qz, kv, kvn, doz, ctxT, lse, dlt, dq, dkv,
        ra, chU, chE, finU, finE,
        ggB, ggC, r1A, r1B, r1C, r2A, r2B, r2C, f3A, f3B, f3C,
        sm, smr, smt, send, recv,
    ) = refs[17:]
    ub, ggA = h2, ggB
    T, D, hs, F = d.tok, d.width, d.span, d.hidden
    nz, nc, nt, nx = d.nz, d.nc, d.nt, d.nx
    heads, B, nb, R, HR, TB = d.heads, d.blk, d.nb, d.rows, d.half, d.tile
    z, c, t = lax.axis_index("fsdp"), lax.axis_index("ctx"), lax.axis_index("tp")
    part = lax.rem(c, 2)
    other = 1 - part
    pair = c + 1 - 2 * part
    core = lax.rem(t, 2)
    xg = t // 2
    mate = t + 1 - 2 * core
    net = Net(send, recv)
    scale = HD ** (-0.5)

    def turn(value, step, size):
        return lax.rem(value + step, size)

    barrier = pltpu.get_barrier_semaphore()
    talks = []
    for rz in range(nz):
        for rc in range(nc):
            if rz or rc:
                talks.append((turn(z, rz, nz), turn(c, rc, nc), t))
    for rt in range(1, nt):
        talks.append((z, c, turn(t, rt, nt)))
    for device in talks:
        pl.semaphore_signal(barrier, inc=1, device_id=device, device_id_type=pl.DeviceIdType.MESH)
    pl.semaphore_wait(barrier, len(talks))

    half_here = pl.ds(pl.multiple_of(part * HR, HR), HR)

    def rows_of(src):
        return pl.ds(pl.multiple_of(src * R + part * HR, HR), HR)

    gathers = []
    for shard, full in ((wa, WA), (wb, WB), (wc, WC)):
        first = [
            net.copy(shard.at[half_here], full.at[rows_of(z)], (turn(z, r, nz), c, t))
            for r in range(1, nz)
        ]
        second = []
        for r in range(1, nz):
            src = turn(z, nz - r, nz)
            second.append(net.copy(full.at[rows_of(src)], full.at[rows_of(src)], (z, pair, t)))
        gathers.append((first, second))
        for one in first:
            one.start()

    def relay(i):
        for one, two in zip(*gathers[i]):
            one.wait_recv()
            two.start()

    def gathered(i):
        for two in gathers[i][1]:
            two.wait_recv()

    sm[...] = jnp.zeros_like(sm)
    g1, b1, g2, b2 = vec[0:1, :], vec[1:2, :], vec[2:3, :], vec[3:4, :]

    def norm_tile(i, carry):
        rows = tile_rows(i, TB)
        xf = x[rows, :].astype(F32)
        mean = jnp.mean(xf, -1, keepdims=True)
        cen = xf - mean
        inv = lax.rsqrt(jnp.mean(cen * cen, -1, keepdims=True) + NORM_EPS)
        normed = cen * inv
        mean_s[rows, :] = mean
        inv_s[rows, :] = inv
        h1[rows, :] = (normed * g1 + b1).astype(BF16)
        h2[rows, :] = (normed * g2 + b2).astype(BF16)
        grad = og[rows, :]
        gb[rows, :] = grad.astype(BF16)
        sm[4:5, :D] += jnp.sum(grad, 0, keepdims=True)
        return carry

    lax.fori_loop(0, T // TB, norm_tile, 0)
    own_rows = pl.ds(pl.multiple_of(z * R, R), R)
    WA[own_rows, :] = wa[...]
    WB[own_rows, :] = wb[...]
    WC[own_rows, :] = wc[...]
    for i in range(nb):
        gbT[i] = jnp.transpose(gb[i * B : (i + 1) * B, :])
        tA[:, i * B : (i + 1) * B] = jnp.transpose(h2[i * B : (i + 1) * B, :])

    relay(0)
    gathered(0)
    WT[...] = jnp.transpose(WA[...])

    for i in range(nb):
        proj = mm_nt(WT[: 3 * hs, :], h1[i * B : (i + 1) * B, :]) + bq[...]
        cb, sb = cosr[i], sinr[i]

        def rotated(tensor):
            lo, hi = tensor[:HALF], tensor[HALF:ROT]
            return jnp.concatenate([lo * cb - hi * sb, hi * cb + lo * sb, tensor[ROT:]], 0)

        own = c * nb + i
        for h in range(heads):
            q = rotated(proj[h * HD : (h + 1) * HD]).astype(BF16) * jnp.asarray(scale, BF16)
            qz[i, h] = jnp.concatenate([q, jnp.zeros_like(q)], 0)
            key = rotated(proj[hs + h * HD : hs + (h + 1) * HD]).astype(BF16)
            value = proj[2 * hs + h * HD : 2 * hs + (h + 1) * HD].astype(BF16)
            both = jnp.concatenate([key, value], 0)
            kv[own, h] = both
            if d.keep:
                kvn[own, h] = jnp.transpose(both)

    own_blocks = pl.ds(c * nb, nb)
    kv_out = [
        net.copy(kv.at[own_blocks], kv.at[own_blocks], (z, turn(c, r, nc), t))
        for r in range(1, nc)
    ]
    for r, one in enumerate(kv_out, 1):

        @pl.when(c + r < nc)
        def _(one=one):
            one.start()

    relay(1)

    for i in range(nb):
        dct = mm(WT[3 * hs :, :], gbT[i]).astype(BF16)
        for h in range(heads):
            piece = dct[h * HD : (h + 1) * HD]
            doz[i, h] = jnp.concatenate([jnp.zeros_like(piece), piece], 0)

    relay(2)
    gathered(1)
    gathered(2)

    def normed_of(rows):
        return (x[rows, :].astype(F32) - mean_s[rows, :]) * inv_s[rows, :]

    def mlp_tile(i, carry):
        rows = tile_rows(i, TB)
        pre = mm(h2[rows, :], WB[...]) + bf1[...]
        cdf = 0.5 * (1.0 + lax.erf(pre * INV_ROOT_TWO))
        density = jnp.exp(-0.5 * pre * pre) * INV_ROOT_TWO_PI
        actb = (pre * cdf).astype(BF16)
        act[rows, :] = actb
        dp = mm(gb[rows, :], WC[...]) * (cdf + pre * density)
        sm[5:6, :F] += jnp.sum(dp, 0, keepdims=True)
        dpb = dp.astype(BF16)
        dpre[rows, :] = dpb
        out[rows, :] = mm_nt(actb, WC[...])
        dh2 = mm_nt(dpb, WB[...])
        sm[2:3, :D] += jnp.sum(dh2 * normed_of(rows), 0, keepdims=True)
        sm[3:4, :D] += jnp.sum(dh2, 0, keepdims=True)
        ig[rows, :] = dh2 * g2
        return carry

    lax.fori_loop(0, T // TB, mlp_tile, 0)

    def store_grad(gg, value, z0):
        for k in range(value.shape[0] // HR):
            gg[k % 2, z0 + k // 2] = value[k * HR : (k + 1) * HR].astype(BF16)

    class Reduce:
        def __init__(self, gg, r1, r2, f3, final):
            self.gg, self.r1, self.r2, self.f3, self.final = gg, r1, r2, f3, final
            self.a = net.copy(gg.at[other], r1, (z, pair, t))
            self.b = [
                net.copy(gg.at[part, turn(z, r, nz)], r2.at[r - 1], (turn(z, r, nz), c, t))
                for r in range(1, nz)
            ]
            self.c = [net.copy(f3.at[c], f3.at[c], (z, turn(c, r, nc), t)) for r in range(1, nc)]

        def one(self):
            self.a.start()

        def two(self):
            self.a.wait_recv()
            for r in range(1, nz):
                zz = turn(z, r, nz)
                self.gg[part, zz] = (self.gg[part, zz].astype(F32) + self.r1[zz].astype(F32)).astype(BF16)
                self.b[r - 1].start()

        def three(self):
            total = self.gg[part, z].astype(F32) + self.r1[z].astype(F32)
            for r in range(1, nz):
                self.b[r - 1].wait_recv()
                total += self.r2[r - 1].astype(F32)
            self.f3[c] = total.astype(BF16)
            for one in self.c:
                one.start()

        def four(self):
            for one in self.c:
                one.wait_recv()
            for p in range(2):
                total = self.f3[p].astype(F32)
                for j in range(1, nc // 2):
                    total += self.f3[2 * j + p].astype(F32)
                self.final[p * HR : (p + 1) * HR, :] = total

        def drain(self):
            for one in [self.a, *self.b, *self.c]:
                one.wait_send()

    redB = Reduce(ggB, r1B, r2B, f3B, gb_out)
    redC = Reduce(ggC, r1C, r2C, f3C, gc_out)
    redA = Reduce(ggA, r1A, r2A, f3A, ga)

    for z0 in range(0, nz, 2):
        store_grad(ggB, mm(tA[z0 * R : (z0 + 2) * R, :], dpre[...]), z0)
    redB.one()
    for z0 in range(0, nz, 2):
        value = None
        for i in range(nb):
            term = mm(gbT[i, z0 * R : (z0 + 2) * R, :], act[i * B : (i + 1) * B, :])
            value = term if value is None else value + term
        store_grad(ggC, value, z0)
    redC.one()

    for r, one in enumerate(kv_out, 1):

        @pl.when(c >= r)
        def _(r=r, one=one):
            one.wait_recv()

            def flip(j, carry):
                at = (c - r) * nb + j
                for h in range(heads):
                    kvn[at, h] = jnp.transpose(kv[at, h])
                return carry

            if d.keep:
                lax.fori_loop(0, nb, flip, 0)

    def natural(at, h):
        return kvn[at, h] if d.keep else jnp.transpose(kv[at, h])

    def allowed_of(i, at):
        query_at = (c * nb + i) * B + lax.broadcasted_iota(jnp.int32, (1, B), 1)
        key_at = at * B + lax.broadcasted_iota(jnp.int32, (B, 1), 0)
        return (key_at <= query_at) & (key_at >= query_at - pos[i])

    for i in range(nb):
        here = c * nb + i
        first_key = jnp.where(here >= d.tail, d.tail, 0)
        for h in range(heads):
            qh = qz[i, h]

            def key_step(at, carry, i=i, h=h, qh=qh):
                top, total, weighted = carry
                s = jnp.where(allowed_of(i, at), mm(natural(at, h), qh), NEG_FILL)
                new_top = jnp.maximum(top, jnp.max(s, 0, keepdims=True))
                w = jnp.exp(s - new_top)
                factor = jnp.exp(top - new_top)
                total = total * factor + jnp.sum(w, 0, keepdims=True)
                weighted = weighted * factor + mm(kv[at, h, HD:], w.astype(BF16))
                return new_top, total, weighted

            top, total, weighted = lax.fori_loop(
                first_key,
                here + 1,
                key_step,
                (
                    jnp.full((1, B), NEG_FILL, F32),
                    jnp.zeros((1, B), F32),
                    jnp.zeros((HD, B), F32),
                ),
            )
            lse[i, h : h + 1, :] = top + jnp.log(total)
            ctx_h = (weighted / total).astype(BF16)
            ctxT[i, h * HD : (h + 1) * HD, :] = ctx_h
            dlt[i, h : h + 1, :] = jnp.sum(
                doz[i, h, HD:].astype(F32) * ctx_h.astype(F32), 0, keepdims=True
            )

    class Join:
        def __init__(self, ra, ch, fin):
            self.ra, self.ch, self.fin = ra, ch, fin
            self.near = net.copy(
                ub.at[pl.ds(pl.multiple_of((1 - core) * (T // 2), T // 2), T // 2)], ra, (z, c, mate)
            )
            self.far = [
                net.copy(ch.at[xg], ch.at[xg], (z, c, turn(xg, r, nx) * 2 + core))
                for r in range(1, nx)
            ]
            self.back = net.copy(fin.at[core], fin.at[core], (z, c, mate))

        def one(self):
            self.near.start()

        def two(self):
            self.near.wait_recv()
            for k in range(T // 2 // TB):
                mine = pl.ds(pl.multiple_of(core * (T // 2) + k * TB, TB), TB)
                tile = slice(k * TB, (k + 1) * TB)
                self.ch[xg, tile, :] = (
                    ub[mine, :].astype(F32) + self.ra[tile, :].astype(F32)
                ).astype(BF16)
            for one in self.far:
                one.start()

        def three(self):
            for one in self.far:
                one.wait_recv()
            for k in range(T // 2 // TB):
                tile = slice(k * TB, (k + 1) * TB)
                total = self.ch[0, tile, :].astype(F32)
                for j in range(1, nx):
                    total += self.ch[j, tile, :].astype(F32)
                self.fin[core, tile, :] = total.astype(BF16)
            self.back.start()

        def four(self):
            self.back.wait_recv()

        def drain(self):
            for one in [*self.far, self.back]:
                one.wait_send()

    join_u = Join(ra, chU, finU)
    join_e = Join(ra, chE, finE)

    for i in range(nb):
        ctx_n = jnp.transpose(ctxT[i])
        for k in range(B // TB):
            rows = slice(i * B + k * TB, i * B + (k + 1) * TB)
            ub[rows, :] = (
                out[rows, :] + mm(ctx_n[k * TB : (k + 1) * TB], WT[3 * hs :, :])
            ).astype(BF16)
    join_u.one()
    redB.two()
    redC.two()

    dq[...] = jnp.zeros_like(dq)

    def key_back(at, h, put):
        k_t = kv[at, h, :HD]
        k_n = natural(at, h)

        def query_step(i, carry):
            dk, dv = carry
            s = mm(k_n, qz[i, h])
            ok = allowed_of(i, at)
            prob = jnp.where(ok, jnp.exp(s - lse[i, h : h + 1, :]), 0.0)
            dp = mm(k_n, doz[i, h])
            ds = (prob * (dp - dlt[i, h : h + 1, :])).astype(BF16)
            dv = dv + mm_nt(doz[i, h, HD:], prob.astype(BF16))
            dk = dk + mm_nt(qz[i, h, :HD], ds)
            dq[i, h] += mm(k_t, ds)
            return dk, dv

        begin = jnp.maximum(at - c * nb, 0)
        end = jnp.where(at < d.tail, jnp.minimum(nb, d.tail - c * nb), nb)
        zero = jnp.zeros((HD, B), F32)
        put(lax.fori_loop(begin, end, query_step, (zero, zero)))

    dkv_out = []
    for r in range(1, nc):
        owner = turn(c, nc - r, nc)
        dkv_out.append(net.copy(kv.at[pl.ds(owner * nb, nb)], kv.at[own_blocks], (z, owner, t)))
    for r in reversed(range(1, nc)):

        @pl.when(c >= r)
        def _(r=r):
            def block(j, carry):
                for h in range(heads):

                    def put(pieces, h=h):
                        kv[(c - r) * nb + j, h, :HD] = pieces[0].astype(BF16)
                        kv[(c - r) * nb + j, h, HD:] = pieces[1].astype(BF16)

                    key_back((c - r) * nb + j, h, put)
                return carry

            lax.fori_loop(0, nb, block, 0)
            dkv_out[r - 1].start()

    join_u.two()

    def own_block(j, carry):
        for h in range(heads):

            def put(pieces, h=h):
                dkv[j, h, :HD] = pieces[0]
                dkv[j, h, HD:] = pieces[1]

            key_back(c * nb + j, h, put)
        return carry

    lax.fori_loop(0, nb, own_block, 0)
    redB.three()
    redC.three()
    join_u.three()

    for r in range(1, nc):

        @pl.when(c + r < nc)
        def _(r=r):
            dkv_out[r - 1].wait_recv()
            for j in range(nb):
                for h in range(heads):
                    dkv[j, h] += kv[(c + r) * nb + j, h].astype(F32)

    grad_t = None
    bias_t = jnp.zeros((3 * hs, 1), F32)
    for i in range(nb):
        cb, sb = cosr[i], sinr[i]

        def unrotated(g):
            lo, hi = g[:HALF], g[HALF:ROT]
            return jnp.concatenate([lo * cb + hi * sb, hi * cb - lo * sb, g[ROT:]], 0)

        pieces = [unrotated(dq[i, h] * scale) for h in range(heads)]
        pieces += [unrotated(dkv[i, h, :HD]) for h in range(heads)]
        pieces += [dkv[i, h, HD:] for h in range(heads)]
        d_proj = jnp.concatenate(pieces, 0)
        bias_t += jnp.sum(d_proj, -1, keepdims=True)
        d_proj_b = d_proj.astype(BF16)
        tA[: 3 * hs, i * B : (i + 1) * B] = d_proj_b
        act[i * B : (i + 1) * B, : 3 * hs] = jnp.transpose(d_proj_b)
    sm[6:7, : 3 * hs] = jnp.transpose(jnp.broadcast_to(bias_t, (3 * hs, 128)))[0:1, :]

    grad_q = mm(tA[: 3 * hs, :], h1[...])
    grad_o = None
    for i in range(nb):
        term = mm(ctxT[i], gb[i * B : (i + 1) * B, :])
        grad_o = term if grad_o is None else grad_o + term
    grad_a = jnp.transpose(jnp.concatenate([grad_q.astype(BF16), grad_o.astype(BF16)], 0))
    for one in [redB.a, *redB.b]:
        one.wait_send()
    store_grad(ggA, grad_a, 0)
    redA.one()
    join_u.near.wait_send()

    def e_tile(i, carry):
        rows = tile_rows(i, TB)
        dh1 = mm(act[rows, : 3 * hs], WT[: 3 * hs, :])
        sm[0:1, :D] += jnp.sum(dh1 * normed_of(rows), 0, keepdims=True)
        sm[1:2, :D] += jnp.sum(dh1, 0, keepdims=True)
        ub[rows, :] = (ig[rows, :] + dh1 * g1).astype(BF16)
        return carry

    lax.fori_loop(0, T // TB, e_tile, 0)
    join_u.four()
    join_e.one()

    rank = z * nc + c
    smr[rank] = sm[...]
    small_a = []
    for rz in range(nz):
        for rc in range(nc):
            if rz or rc:
                small_a.append(
                    net.copy(smr.at[rank], smr.at[rank], (turn(z, rz, nz), turn(c, rc, nc), t))
                )
    for one in small_a:
        one.start()
    join_e.two()
    redA.two()

    def out_tile(i, carry):
        rows = tile_rows(i, TB)
        per = T // 2 // TB
        total = finU[i // per, tile_rows(lax.rem(i, per), TB), :].astype(F32)
        out[rows, :] = x[rows, :].astype(F32) + total + vec[4:5, :]
        return carry

    lax.fori_loop(0, T // TB, out_tile, 0)
    redB.four()
    redC.four()

    for one in small_a:
        one.wait_recv()
    tot = smr[0]
    for j in range(1, nz * nc):
        tot += smr[j]
    smt[t] = tot
    small_b = [net.copy(smt.at[t], smt.at[t], (z, c, turn(t, r, nt))) for r in range(1, nt)]
    for one in small_b:
        one.start()
    redA.three()
    join_e.three()
    for one in small_b:
        one.wait_recv()
    tops = smt[0, 0:4, :]
    for j in range(1, nt):
        tops += smt[j, 0:4, :]
    sm_out[...] = jnp.concatenate([tops, tot[4:8, :]], 0)
    join_e.four()

    def in_tile(i, carry):
        rows = tile_rows(i, TB)
        per = T // 2 // TB
        e = finE[i // per, tile_rows(lax.rem(i, per), TB), :].astype(F32)
        normed = normed_of(rows)
        ig[rows, :] = og[rows, :] + inv_s[rows, :] * (
            e
            - jnp.mean(e, -1, keepdims=True)
            - normed * jnp.mean(e * normed, -1, keepdims=True)
        )
        return carry

    lax.fori_loop(0, T // TB, in_tile, 0)
    redA.four()

    for first, second in gathers:
        for one in [*first, *second]:
            one.wait_send()
    for r, one in enumerate(kv_out, 1):

        @pl.when(c + r < nc)
        def _(one=one):
            one.wait_send()

    for r, one in enumerate(dkv_out, 1):

        @pl.when(c >= r)
        def _(one=one):
            one.wait_send()

    for one in redB.c:
        one.wait_send()
    redA.drain()
    redC.drain()
    join_u.drain()
    join_e.near.wait_send()
    join_e.drain()
    for one in [*small_a, *small_b]:
        one.wait_send()
    assert net.used == d.n_copies


def body(
    mesh,
    layer_input,
    segments,
    positions,
    ln1_gain,
    ln1_bias,
    ln2_gain,
    ln2_bias,
    w_qkv,
    b_qkv,
    w_out,
    b_out,
    w_fc1,
    b_fc1,
    w_fc2,
    b_fc2,
    out_grad,
):
    d = Dims(mesh, layer_input.shape[0], layer_input.shape[1], b_qkv.shape[1], b_fc1.shape[0])
    T, D, hs, F, B, nb = d.tok, d.width, d.span, d.hidden, d.blk, d.nb
    R, HR, nz, nc = d.rows, d.half, d.nz, d.nc
    freqs = 10000.0 ** (-(jnp.arange(HALF, dtype=F32) * 2.0) / ROT)
    angles = positions.astype(F32).reshape(nb, 1, B) * freqs[None, :, None]
    vec = jnp.stack([ln1_gain, ln1_bias, ln2_gain, ln2_bias, b_out + b_fc2] + [ln1_gain] * 3)
    wide_a = 4 * hs
    args = (
        layer_input,
        out_grad,
        positions.reshape(nb, 1, B),
        jnp.cos(angles),
        jnp.sin(angles),
        vec,
        b_qkv.reshape(3 * hs, 1),
        b_fc1.reshape(1, F),
        jnp.concatenate([w_qkv.reshape(R, 3 * hs), w_out.T], 1),
        w_fc1,
        w_fc2.T,
    )
    vm = pltpu.VMEM
    h, W = d.heads, d.wide
    scratch = [
        vm((D, wide_a), BF16), vm((D, F), BF16), vm((D, F), BF16), vm((wide_a, D), BF16),
        vm((T, D), BF16), vm((T, D), BF16), vm((D, T), BF16), vm((T, D), BF16), vm((nb, D, B), BF16),
        vm((T, 1), F32), vm((T, 1), F32), vm((T, F), BF16), vm((T, F), BF16),
        vm((nb, h, 2 * HD, B), BF16), vm((d.nkb, h, 2 * HD, B), BF16), vm((d.nkb if d.keep else 1, h, B, 2 * HD), BF16),
        vm((nb, h, 2 * HD, B), BF16), vm((nb, hs, B), BF16),
        vm((nb, 8, B), F32), vm((nb, 8, B), F32), vm((nb, h, HD, B), F32),
        vm((nb, h, 2 * HD, B), F32),
        vm((T // 2, D), BF16),
        vm((d.nx, T // 2, D), BF16), vm((d.nx, T // 2, D), BF16),
        vm((2, T // 2, D), BF16), vm((2, T // 2, D), BF16),
    ]
    widths = (wide_a, F, F)
    scratch += [vm((2, nz, HR, w), BF16) for w in widths[1:]]
    scratch += [vm((nz, HR, w), BF16) for w in widths]
    scratch += [vm((nz - 1, HR, w), BF16) for w in widths]
    scratch += [vm((nc, HR, w), BF16) for w in widths]
    scratch += [vm((8, W), F32), vm((nz * nc, 8, W), F32), vm((d.nt, 8, W), F32)]
    scratch += [pltpu.SemaphoreType.DMA((d.n_copies,)), pltpu.SemaphoreType.DMA((d.n_copies,))]

    def kernel(*refs):
        layer_kernel(d, *refs)

    out, ig, ga, gb, gc, small = pl.pallas_call(
        kernel,
        out_shape=(
            jax.ShapeDtypeStruct((T, D), F32),
            jax.ShapeDtypeStruct((T, D), F32),
            jax.ShapeDtypeStruct((R, wide_a), F32),
            jax.ShapeDtypeStruct((R, F), F32),
            jax.ShapeDtypeStruct((R, F), F32),
            jax.ShapeDtypeStruct((8, W), F32),
        ),
        in_specs=[pl.BlockSpec(memory_space=vm)] * len(args),
        out_specs=[pl.BlockSpec(memory_space=vm)] * 6,
        scratch_shapes=scratch,
        compiler_params=pltpu.CompilerParams(
            collective_id=0, has_side_effects=True, vmem_limit_bytes=VMEM_BYTES
        ),
    )(*args)
    return (
        out,
        ig,
        small[0, :D],
        small[1, :D],
        small[2, :D],
        small[3, :D],
        ga[:, : 3 * hs].reshape(R, 3, hs),
        small[6, : 3 * hs].reshape(3, hs),
        ga[:, 3 * hs :].T,
        small[4, :D],
        gb,
        small[5, :F],
        gc.T,
        small[4, :D],
    )


def solution(mesh):
    in_specs = (
        P(("fsdp", "ctx"), None),
        P("fsdp"),
        P(("fsdp", "ctx")),
        P(),
        P(),
        P(),
        P(),
        P("fsdp", None, "tp"),
        P(None, "tp"),
        P("tp", "fsdp"),
        P(),
        P("fsdp", "tp"),
        P("tp"),
        P("tp", "fsdp"),
        P(),
        P(("fsdp", "ctx"), None),
    )
    out_specs = (
        P(("fsdp", "ctx"), None),
        P(("fsdp", "ctx"), None),
        P(),
        P(),
        P(),
        P(),
        P("fsdp", None, "tp"),
        P(None, "tp"),
        P("tp", "fsdp"),
        P(),
        P("fsdp", "tp"),
        P("tp"),
        P("tp", "fsdp"),
        P(),
    )

    def step(*args):
        return body(mesh, *args)

    return jax.shard_map(step, mesh=mesh, in_specs=in_specs, out_specs=out_specs, check_vma=False)
```

```python
import math

import jax
import jax.numpy as jnp
from jax import lax
from jax.experimental import pallas as pl
from jax.experimental.pallas import tpu as pltpu
from jax.sharding import PartitionSpec as P

HD = 64
ROT = 16
HALF = ROT // 2
NEG_FILL = -1e30
NORM_EPS = 1e-05
INV_ROOT_TWO = 0.7071067811865476
INV_ROOT_TWO_PI = 0.3989422804014327
F32 = jnp.float32
BF16 = jnp.bfloat16
VMEM_BYTES = 67043328


def mm(a, b):
    return jnp.dot(a, b, preferred_element_type=F32)


def mm_nt(a, b):
    return lax.dot_general(a, b, (((1,), (1,)), ((), ())), preferred_element_type=F32)


def tile_rows(i, size):
    return pl.ds(pl.multiple_of(i * size, size), size)


class Dims:
    def __init__(self, mesh, tokens, width, span, hidden):
        self.nz, self.nc, self.nt = mesh.shape["fsdp"], mesh.shape["ctx"], mesh.shape["tp"]
        self.tok, self.width, self.span, self.hidden = tokens, width, span, hidden
        self.heads = span // HD
        self.blk = min(512, tokens)
        self.nb = tokens // self.blk
        self.nkb = self.nc * self.nb
        self.tail = (3 * self.nkb) // 4
        self.rows = width // self.nz
        self.half = self.rows // 2
        self.tile = min(256, tokens)
        self.nx = self.nt // 2
        self.keep = self.nc <= 2
        assert 4 * span == hidden and self.nt % 2 == 0 and self.nc % 2 == 0
        self.wide = max(width, hidden, 3 * span)
        nz, nc, nx = self.nz, self.nc, self.nx
        self.n_copies = (
            3 * 2 * (nz - 1)
            + 2 * (nc - 1)
            + 2 * (nx + 1)
            + 3 * (1 + (nz - 1) + (nc - 1))
            + (nz * nc - 1)
            + (self.nt - 1)
        )


class Net:
    def __init__(self, send, recv):
        self.send, self.recv, self.used, self.started = send, recv, 0, []

    def copy(self, src, dst, device):
        i = self.used
        self.used += 1
        return pltpu.make_async_remote_copy(
            src_ref=src,
            dst_ref=dst,
            send_sem=self.send.at[i],
            recv_sem=self.recv.at[i],
            device_id=device,
            device_id_type=pl.DeviceIdType.MESH,
        )


def layer_kernel(d, *refs):
    (x, og, pos_in, gain1, shift1, gain2, shift2, bq_in, bf_in, wq_in, wo_in, wb, wc) = refs[:13]
    (u_out, e_out, ga_out, gb_out, gc_out, sm_out) = refs[13:19]
    (
        WA, WB, WC, WT, h1, h2, tA, gb, gbT, mean_s, inv_s, act, dpre,
        qz, kv, kvn, doz, ctxT, lse, dlt, dq, dkv,
        ra, chU, chE, finU, finE,
        ggB, ggC, r1A, r1B, r1C, r2A, r2B, r2C, f3A, f3B, f3C,
        sm, smr, smt, out, ig, wa, cosr, sinr, pos, send, recv, local,
    ) = refs[19:]
    ub, ggA = h2, ggB
    T, D, hs, F = d.tok, d.width, d.span, d.hidden
    nz, nc, nt, nx = d.nz, d.nc, d.nt, d.nx
    heads, B, nb, R, HR, TB = d.heads, d.blk, d.nb, d.rows, d.half, d.tile
    z, c, t = lax.axis_index("fsdp"), lax.axis_index("ctx"), lax.axis_index("tp")
    part = lax.rem(c, 2)
    other = 1 - part
    pair = c + 1 - 2 * part
    core = lax.rem(t, 2)
    xg = t // 2
    mate = t + 1 - 2 * core
    net = Net(send, recv)
    scale = HD ** (-0.5)

    def turn(value, step, size):
        return lax.rem(value + step, size)

    barrier = pltpu.get_barrier_semaphore()
    talks = []
    for rz in range(nz):
        for rc in range(nc):
            if rz or rc:
                talks.append((turn(z, rz, nz), turn(c, rc, nc), t))
    for rt in range(1, nt):
        talks.append((z, c, turn(t, rt, nt)))
    for device in talks:
        pl.semaphore_signal(barrier, inc=1, device_id=device, device_id_type=pl.DeviceIdType.MESH)
    pl.semaphore_wait(barrier, len(talks))

    half_here = pl.ds(pl.multiple_of(part * HR, HR), HR)

    def rows_of(src):
        return pl.ds(pl.multiple_of(src * R + part * HR, HR), HR)

    gathers = []
    wa[...] = jnp.concatenate([wq_in[0], wq_in[1], wq_in[2], jnp.transpose(wo_in[...])], 1)
    for shard, full in ((wa, WA), (wb, WB), (wc, WC)):
        first = [
            net.copy(shard.at[half_here], full.at[rows_of(z)], (turn(z, r, nz), c, t))
            for r in range(1, nz)
        ]
        second = []
        for r in range(1, nz):
            src = turn(z, nz - r, nz)
            second.append(net.copy(full.at[rows_of(src)], full.at[rows_of(src)], (z, pair, t)))
        gathers.append((first, second))
        for one in first:
            one.start()

    def relay(i):
        for one, two in zip(*gathers[i]):
            one.wait_recv()
            two.start()

    def gathered(i):
        for two in gathers[i][1]:
            two.wait_recv()

    sm[...] = jnp.zeros_like(sm)
    g1, b1, g2, b2 = [one[...].reshape(1, D) for one in (gain1, shift1, gain2, shift2)]
    bf1 = bf_in[...].reshape(1, F)
    positions = pos_in[...].reshape(1, T)
    exponent = lax.broadcasted_iota(jnp.int32, (HALF, 1), 0).astype(F32) * (-2.0 / ROT)
    freqs = jnp.exp(exponent * math.log(10000.0))
    for i in range(nb):
        pos[i] = positions[:, i * B : (i + 1) * B]
        angle = pos[i].astype(F32) * freqs
        cosr[i] = jnp.cos(angle)
        sinr[i] = jnp.sin(angle)
    bq = jnp.concatenate(
        [jnp.transpose(jnp.broadcast_to(bq_in[j : j + 1, :], (128, hs)))[:, :1] for j in range(3)], 0
    )

    def norm_tile(i, carry):
        rows = tile_rows(i, TB)
        xf = x[rows, :].astype(F32)
        mean = jnp.mean(xf, -1, keepdims=True)
        cen = xf - mean
        inv = lax.rsqrt(jnp.mean(cen * cen, -1, keepdims=True) + NORM_EPS)
        normed = cen * inv
        mean_s[rows, :] = mean
        inv_s[rows, :] = inv
        h1[rows, :] = (normed * g1 + b1).astype(BF16)
        h2[rows, :] = (normed * g2 + b2).astype(BF16)
        grad = og[rows, :]
        gb[rows, :] = grad.astype(BF16)
        sm[4:5, :D] += jnp.sum(grad, 0, keepdims=True)
        return carry

    lax.fori_loop(0, T // TB, norm_tile, 0)
    own_rows = pl.ds(pl.multiple_of(z * R, R), R)
    WA[own_rows, :] = wa[...]
    WB[own_rows, :] = wb[...]
    WC[own_rows, :] = wc[...]
    for i in range(nb):
        gbT[i] = jnp.transpose(gb[i * B : (i + 1) * B, :])
        tA[:, i * B : (i + 1) * B] = jnp.transpose(h2[i * B : (i + 1) * B, :])

    relay(0)
    gathered(0)
    WT[...] = jnp.transpose(WA[...])

    for i in range(nb):
        proj = mm_nt(WT[: 3 * hs, :], h1[i * B : (i + 1) * B, :]) + bq
        cb, sb = cosr[i], sinr[i]

        def rotated(tensor):
            lo, hi = tensor[:HALF], tensor[HALF:ROT]
            return jnp.concatenate([lo * cb - hi * sb, hi * cb + lo * sb, tensor[ROT:]], 0)

        own = c * nb + i
        for h in range(heads):
            q = rotated(proj[h * HD : (h + 1) * HD]).astype(BF16) * jnp.asarray(scale, BF16)
            qz[i, h] = jnp.concatenate([q, jnp.zeros_like(q)], 0)
            key = rotated(proj[hs + h * HD : hs + (h + 1) * HD]).astype(BF16)
            value = proj[2 * hs + h * HD : 2 * hs + (h + 1) * HD].astype(BF16)
            both = jnp.concatenate([key, value], 0)
            kv[own, h] = both
            if d.keep:
                kvn[own, h] = jnp.transpose(both)

    own_blocks = pl.ds(c * nb, nb)
    kv_out = [
        net.copy(kv.at[own_blocks], kv.at[own_blocks], (z, turn(c, r, nc), t))
        for r in range(1, nc)
    ]
    for r, one in enumerate(kv_out, 1):

        @pl.when(c + r < nc)
        def _(one=one):
            one.start()

    relay(1)

    for i in range(nb):
        dct = mm(WT[3 * hs :, :], gbT[i]).astype(BF16)
        for h in range(heads):
            piece = dct[h * HD : (h + 1) * HD]
            doz[i, h] = jnp.concatenate([jnp.zeros_like(piece), piece], 0)

    relay(2)
    gathered(1)
    gathered(2)

    def normed_of(rows):
        return (x[rows, :].astype(F32) - mean_s[rows, :]) * inv_s[rows, :]

    def mlp_tile(i, carry):
        rows = tile_rows(i, TB)
        pre = mm(h2[rows, :], WB[...]) + bf1
        cdf = 0.5 * (1.0 + lax.erf(pre * INV_ROOT_TWO))
        density = jnp.exp(-0.5 * pre * pre) * INV_ROOT_TWO_PI
        actb = (pre * cdf).astype(BF16)
        act[rows, :] = actb
        dp = mm(gb[rows, :], WC[...]) * (cdf + pre * density)
        sm[5:6, :F] += jnp.sum(dp, 0, keepdims=True)
        dpb = dp.astype(BF16)
        dpre[rows, :] = dpb
        out[rows, :] = mm_nt(actb, WC[...])
        dh2 = mm_nt(dpb, WB[...])
        sm[2:3, :D] += jnp.sum(dh2 * normed_of(rows), 0, keepdims=True)
        sm[3:4, :D] += jnp.sum(dh2, 0, keepdims=True)
        ig[rows, :] = dh2 * g2
        return carry

    lax.fori_loop(0, T // TB, mlp_tile, 0)

    def store_grad(gg, value, z0):
        for k in range(value.shape[0] // HR):
            gg[k % 2, z0 + k // 2] = value[k * HR : (k + 1) * HR].astype(BF16)

    class Reduce:
        def __init__(self, i, gg, r1, r2, f3, final):
            self.gg, self.r1, self.r2, self.f3 = gg, r1, r2, f3
            self.put = pltpu.make_async_copy(f3, final, local.at[i])
            self.a = net.copy(gg.at[other], r1, (z, pair, t))
            self.b = [
                net.copy(gg.at[part, turn(z, r, nz)], r2.at[r - 1], (turn(z, r, nz), c, t))
                for r in range(1, nz)
            ]
            self.c = [net.copy(f3.at[c], f3.at[c], (z, turn(c, r, nc), t)) for r in range(1, nc)]

        def one(self):
            self.a.start()

        def two(self):
            self.a.wait_recv()
            for r in range(1, nz):
                zz = turn(z, r, nz)
                self.gg[part, zz] = (self.gg[part, zz].astype(F32) + self.r1[zz].astype(F32)).astype(BF16)
                self.b[r - 1].start()

        def three(self):
            total = self.gg[part, z].astype(F32) + self.r1[z].astype(F32)
            for r in range(1, nz):
                self.b[r - 1].wait_recv()
                total += self.r2[r - 1].astype(F32)
            self.f3[c] = total.astype(BF16)
            for one in self.c:
                one.start()

        def four(self):
            for one in self.c:
                one.wait_recv()
            self.put.start()

        def drain(self):
            for one in [self.a, *self.b, *self.c]:
                one.wait_send()

    redB = Reduce(0, ggB, r1B, r2B, f3B, gb_out)
    redC = Reduce(1, ggC, r1C, r2C, f3C, gc_out)
    redA = Reduce(2, ggA, r1A, r2A, f3A, ga_out)

    for z0 in range(0, nz, 2):
        store_grad(ggB, mm(tA[z0 * R : (z0 + 2) * R, :], dpre[...]), z0)
    redB.one()
    for z0 in range(0, nz, 2):
        value = None
        for i in range(nb):
            term = mm(gbT[i, z0 * R : (z0 + 2) * R, :], act[i * B : (i + 1) * B, :])
            value = term if value is None else value + term
        store_grad(ggC, value, z0)
    redC.one()

    for r, one in enumerate(kv_out, 1):

        @pl.when(c >= r)
        def _(r=r, one=one):
            one.wait_recv()

            def flip(j, carry):
                at = (c - r) * nb + j
                for h in range(heads):
                    kvn[at, h] = jnp.transpose(kv[at, h])
                return carry

            if d.keep:
                lax.fori_loop(0, nb, flip, 0)

    def natural(at, h):
        return kvn[at, h] if d.keep else jnp.transpose(kv[at, h])

    def allowed_of(i, at):
        query_at = (c * nb + i) * B + lax.broadcasted_iota(jnp.int32, (1, B), 1)
        key_at = at * B + lax.broadcasted_iota(jnp.int32, (B, 1), 0)
        return (key_at <= query_at) & (key_at >= query_at - pos[i])

    for i in range(nb):
        here = c * nb + i
        first_key = jnp.where(here >= d.tail, d.tail, 0)
        for h in range(heads):
            qh = qz[i, h]

            def key_step(at, carry, i=i, h=h, qh=qh):
                top, total, weighted = carry
                s = jnp.where(allowed_of(i, at), mm(natural(at, h), qh), NEG_FILL)
                new_top = jnp.maximum(top, jnp.max(s, 0, keepdims=True))
                w = jnp.exp(s - new_top)
                factor = jnp.exp(top - new_top)
                total = total * factor + jnp.sum(w, 0, keepdims=True)
                weighted = weighted * factor + mm(kv[at, h, HD:], w.astype(BF16))
                return new_top, total, weighted

            top, total, weighted = lax.fori_loop(
                first_key,
                here + 1,
                key_step,
                (
                    jnp.full((1, B), NEG_FILL, F32),
                    jnp.zeros((1, B), F32),
                    jnp.zeros((HD, B), F32),
                ),
            )
            lse[i, h : h + 1, :] = top + jnp.log(total)
            ctx_h = (weighted / total).astype(BF16)
            ctxT[i, h * HD : (h + 1) * HD, :] = ctx_h
            dlt[i, h : h + 1, :] = jnp.sum(
                doz[i, h, HD:].astype(F32) * ctx_h.astype(F32), 0, keepdims=True
            )

    class Join:
        def __init__(self, ra, ch, fin):
            self.ra, self.ch, self.fin = ra, ch, fin
            self.near = net.copy(
                ub.at[pl.ds(pl.multiple_of((1 - core) * (T // 2), T // 2), T // 2)], ra, (z, c, mate)
            )
            self.far = [
                net.copy(ch.at[xg], ch.at[xg], (z, c, turn(xg, r, nx) * 2 + core))
                for r in range(1, nx)
            ]
            self.back = net.copy(fin.at[core], fin.at[core], (z, c, mate))

        def one(self):
            self.near.start()

        def two(self):
            self.near.wait_recv()
            for k in range(T // 2 // TB):
                mine = pl.ds(pl.multiple_of(core * (T // 2) + k * TB, TB), TB)
                tile = slice(k * TB, (k + 1) * TB)
                self.ch[xg, tile, :] = (
                    ub[mine, :].astype(F32) + self.ra[tile, :].astype(F32)
                ).astype(BF16)
            for one in self.far:
                one.start()

        def three(self):
            for one in self.far:
                one.wait_recv()
            for k in range(T // 2 // TB):
                tile = slice(k * TB, (k + 1) * TB)
                total = self.ch[0, tile, :].astype(F32)
                for j in range(1, nx):
                    total += self.ch[j, tile, :].astype(F32)
                self.fin[core, tile, :] = total.astype(BF16)
            self.back.start()

        def four(self):
            self.back.wait_recv()

        def drain(self):
            for one in [*self.far, self.back]:
                one.wait_send()

    join_u = Join(ra, chU, finU)
    join_e = Join(ra, chE, finE)

    for i in range(nb):
        ctx_n = jnp.transpose(ctxT[i])
        for k in range(B // TB):
            rows = slice(i * B + k * TB, i * B + (k + 1) * TB)
            ub[rows, :] = (
                out[rows, :] + mm(ctx_n[k * TB : (k + 1) * TB], WT[3 * hs :, :])
            ).astype(BF16)
    join_u.one()
    redB.two()
    redC.two()

    dq[...] = jnp.zeros_like(dq)

    def key_back(at, h, put):
        k_t = kv[at, h, :HD]
        k_n = natural(at, h)

        def query_step(i, carry):
            dk, dv = carry
            s = mm(k_n, qz[i, h])
            ok = allowed_of(i, at)
            prob = jnp.where(ok, jnp.exp(s - lse[i, h : h + 1, :]), 0.0)
            dp = mm(k_n, doz[i, h])
            ds = (prob * (dp - dlt[i, h : h + 1, :])).astype(BF16)
            dv = dv + mm_nt(doz[i, h, HD:], prob.astype(BF16))
            dk = dk + mm_nt(qz[i, h, :HD], ds)
            dq[i, h] += mm(k_t, ds)
            return dk, dv

        begin = jnp.maximum(at - c * nb, 0)
        end = jnp.where(at < d.tail, jnp.minimum(nb, d.tail - c * nb), nb)
        zero = jnp.zeros((HD, B), F32)
        put(lax.fori_loop(begin, end, query_step, (zero, zero)))

    dkv_out = []
    for r in range(1, nc):
        owner = turn(c, nc - r, nc)
        dkv_out.append(net.copy(kv.at[pl.ds(owner * nb, nb)], kv.at[own_blocks], (z, owner, t)))
    for r in reversed(range(1, nc)):

        @pl.when(c >= r)
        def _(r=r):
            def block(j, carry):
                for h in range(heads):

                    def put(pieces, h=h):
                        kv[(c - r) * nb + j, h, :HD] = pieces[0].astype(BF16)
                        kv[(c - r) * nb + j, h, HD:] = pieces[1].astype(BF16)

                    key_back((c - r) * nb + j, h, put)
                return carry

            lax.fori_loop(0, nb, block, 0)
            dkv_out[r - 1].start()

    join_u.two()

    def own_block(j, carry):
        for h in range(heads):

            def put(pieces, h=h):
                dkv[j, h, :HD] = pieces[0]
                dkv[j, h, HD:] = pieces[1]

            key_back(c * nb + j, h, put)
        return carry

    lax.fori_loop(0, nb, own_block, 0)
    redB.three()
    redC.three()
    join_u.three()

    for r in range(1, nc):

        @pl.when(c + r < nc)
        def _(r=r):
            dkv_out[r - 1].wait_recv()
            for j in range(nb):
                for h in range(heads):
                    dkv[j, h] += kv[(c + r) * nb + j, h].astype(F32)

    grad_t = None
    bias_t = jnp.zeros((3 * hs, 1), F32)
    for i in range(nb):
        cb, sb = cosr[i], sinr[i]

        def unrotated(g):
            lo, hi = g[:HALF], g[HALF:ROT]
            return jnp.concatenate([lo * cb + hi * sb, hi * cb - lo * sb, g[ROT:]], 0)

        pieces = [unrotated(dq[i, h] * scale) for h in range(heads)]
        pieces += [unrotated(dkv[i, h, :HD]) for h in range(heads)]
        pieces += [dkv[i, h, HD:] for h in range(heads)]
        d_proj = jnp.concatenate(pieces, 0)
        bias_t += jnp.sum(d_proj, -1, keepdims=True)
        d_proj_b = d_proj.astype(BF16)
        tA[: 3 * hs, i * B : (i + 1) * B] = d_proj_b
        act[i * B : (i + 1) * B, : 3 * hs] = jnp.transpose(d_proj_b)
    sm[6:7, : 3 * hs] = jnp.transpose(jnp.broadcast_to(bias_t, (3 * hs, 128)))[0:1, :]

    grad_q = mm(tA[: 3 * hs, :], h1[...])
    grad_o = None
    for i in range(nb):
        term = mm(ctxT[i], gb[i * B : (i + 1) * B, :])
        grad_o = term if grad_o is None else grad_o + term
    grad_a = jnp.transpose(jnp.concatenate([grad_q.astype(BF16), grad_o.astype(BF16)], 0))
    for one in [redB.a, *redB.b]:
        one.wait_send()
    store_grad(ggA, grad_a, 0)
    redA.one()
    join_u.near.wait_send()

    def e_tile(i, carry):
        rows = tile_rows(i, TB)
        dh1 = mm(act[rows, : 3 * hs], WT[: 3 * hs, :])
        sm[0:1, :D] += jnp.sum(dh1 * normed_of(rows), 0, keepdims=True)
        sm[1:2, :D] += jnp.sum(dh1, 0, keepdims=True)
        ub[rows, :] = (ig[rows, :] + dh1 * g1).astype(BF16)
        return carry

    lax.fori_loop(0, T // TB, e_tile, 0)
    join_u.four()
    join_e.one()

    rank = z * nc + c
    smr[rank] = sm[...]
    small_a = []
    for rz in range(nz):
        for rc in range(nc):
            if rz or rc:
                small_a.append(
                    net.copy(smr.at[rank], smr.at[rank], (turn(z, rz, nz), turn(c, rc, nc), t))
                )
    for one in small_a:
        one.start()
    join_e.two()
    redA.two()

    put_u = pltpu.make_async_copy(finU, u_out, local.at[3])
    put_u.start()
    redB.four()
    redC.four()

    for one in small_a:
        one.wait_recv()
    tot = smr[0]
    for j in range(1, nz * nc):
        tot += smr[j]
    smt[t] = tot
    small_b = [net.copy(smt.at[t], smt.at[t], (z, c, turn(t, r, nt))) for r in range(1, nt)]
    for one in small_b:
        one.start()
    redA.three()
    join_e.three()
    for one in small_b:
        one.wait_recv()
    tops = smt[0, 0:4, :]
    for j in range(1, nt):
        tops += smt[j, 0:4, :]
    sm_out[...] = jnp.concatenate([tops, tot[4:8, :]], 0)
    join_e.four()

    put_e = pltpu.make_async_copy(finE, e_out, local.at[4])
    put_e.start()
    redA.four()

    for first, second in gathers:
        for one in [*first, *second]:
            one.wait_send()
    for r, one in enumerate(kv_out, 1):

        @pl.when(c + r < nc)
        def _(one=one):
            one.wait_send()

    for r, one in enumerate(dkv_out, 1):

        @pl.when(c >= r)
        def _(one=one):
            one.wait_send()

    for one in redB.c:
        one.wait_send()
    redA.drain()
    redC.drain()
    join_u.drain()
    join_e.near.wait_send()
    join_e.drain()
    for one in [*small_a, *small_b]:
        one.wait_send()
    for one in (redA.put, redB.put, redC.put, put_u, put_e):
        one.wait()
    assert net.used == d.n_copies


def body(
    mesh,
    layer_input,
    segments,
    positions,
    ln1_gain,
    ln1_bias,
    ln2_gain,
    ln2_bias,
    w_qkv,
    b_qkv,
    w_out,
    b_out,
    w_fc1,
    b_fc1,
    w_fc2,
    b_fc2,
    out_grad,
):
    d = Dims(mesh, layer_input.shape[0], layer_input.shape[1], b_qkv.shape[1], b_fc1.shape[0])
    T, D, hs, F, B, nb = d.tok, d.width, d.span, d.hidden, d.blk, d.nb
    R, HR, nz, nc = d.rows, d.half, d.nz, d.nc
    wide_a = 4 * hs
    args = (
        layer_input,
        out_grad,
        positions,
        ln1_gain,
        ln1_bias,
        ln2_gain,
        ln2_bias,
        b_qkv,
        b_fc1,
        jnp.transpose(w_qkv, (1, 0, 2)),
        w_out,
        w_fc1,
        w_fc2.T,
    )
    vm = pltpu.VMEM
    h, W = d.heads, d.wide
    scratch = [
        vm((D, wide_a), BF16), vm((D, F), BF16), vm((D, F), BF16), vm((wide_a, D), BF16),
        vm((T, D), BF16), vm((T, D), BF16), vm((D, T), BF16), vm((T, D), BF16), vm((nb, D, B), BF16),
        vm((T, 1), F32), vm((T, 1), F32), vm((T, F), BF16), vm((T, F), BF16),
        vm((nb, h, 2 * HD, B), BF16), vm((d.nkb, h, 2 * HD, B), BF16), vm((d.nkb if d.keep else 1, h, B, 2 * HD), BF16),
        vm((nb, h, 2 * HD, B), BF16), vm((nb, hs, B), BF16),
        vm((nb, 8, B), F32), vm((nb, 8, B), F32), vm((nb, h, HD, B), F32),
        vm((nb, h, 2 * HD, B), F32),
        vm((T // 2, D), BF16),
        vm((d.nx, T // 2, D), BF16), vm((d.nx, T // 2, D), BF16),
        vm((2, T // 2, D), BF16), vm((2, T // 2, D), BF16),
    ]
    widths = (wide_a, F, F)
    scratch += [vm((2, nz, HR, w), BF16) for w in widths[1:]]
    scratch += [vm((nz, HR, w), BF16) for w in widths]
    scratch += [vm((nz - 1, HR, w), BF16) for w in widths]
    scratch += [vm((nc, HR, w), BF16) for w in widths]
    scratch += [vm((8, W), F32), vm((nz * nc, 8, W), F32), vm((d.nt, 8, W), F32)]
    scratch += [vm((T, D), F32), vm((T, D), F32), vm((R, wide_a), BF16)]
    scratch += [vm((nb, HALF, B), F32), vm((nb, HALF, B), F32), vm((nb, 1, B), jnp.int32)]
    scratch += [pltpu.SemaphoreType.DMA((n,)) for n in (d.n_copies, d.n_copies, 5)]

    def kernel(*refs):
        layer_kernel(d, *refs)

    fin = jax.ShapeDtypeStruct((2, T // 2, D), BF16)
    sums = [jax.ShapeDtypeStruct((nc, HR, w), BF16) for w in widths]
    in_hbm = pl.BlockSpec(memory_space=pl.ANY)
    joined, joined_e, *owned, small = pl.pallas_call(
        kernel,
        out_shape=(fin, fin, *sums, jax.ShapeDtypeStruct((8, W), F32)),
        in_specs=[pl.BlockSpec(memory_space=vm)] * len(args),
        out_specs=[in_hbm] * 5 + [pl.BlockSpec(memory_space=vm)],
        scratch_shapes=scratch,
        compiler_params=pltpu.CompilerParams(
            collective_id=0, has_side_effects=True, vmem_limit_bytes=VMEM_BYTES
        ),
    )(*args)

    TB = d.tile

    def tiles():
        return pl.BlockSpec((TB, D), lambda i: (i, 0))

    def whole(shape):
        return pl.BlockSpec(shape, lambda i: (0,) * len(shape))

    outs = [
        ((T, D), True), ((T, D), True), ((D,), False), ((D,), False), ((D,), False), ((D,), False),
        ((3, R, hs), False), ((3, hs), False), ((hs, R), False), ((D,), False), ((R, F), False),
        ((F,), False), ((R, F), False), ((D,), False),
    ]
    results = pl.pallas_call(
        lambda *refs: finish_kernel(d, *refs),
        grid=(T // TB,),
        out_shape=[jax.ShapeDtypeStruct(shape, F32) for shape, _ in outs],
        in_specs=[tiles(), tiles(), tiles(), tiles()]
        + [whole(o.shape) for o in owned]
        + [whole((8, W)), whole((D,)), whole((D,))],
        out_specs=[tiles() if tiled else whole(shape) for shape, tiled in outs],
        compiler_params=pltpu.CompilerParams(vmem_limit_bytes=VMEM_BYTES),
    )(
        layer_input, out_grad, joined.reshape(T, D), joined_e.reshape(T, D), *owned, small, b_out, b_fc2
    )
    results = list(results)
    results[6] = jnp.transpose(results[6], (1, 0, 2))
    results[12] = results[12].T
    return tuple(results)


def finish_kernel(d, x, og, u, e, fa, fb, fc, small, bo, bf2, *outs):
    out, ig, o_g1, o_b1, o_g2, o_b2, o_qkv, o_bqkv, o_wo, o_bo, o_fc1, o_bf1, o_fc2, o_bf2 = outs
    D, hs, F, HR = d.width, d.span, d.hidden, d.half
    xf = x[...].astype(F32)
    out[...] = xf + u[...].astype(F32) + (bo[...] + bf2[...]).reshape(1, D)
    cen = xf - jnp.mean(xf, -1, keepdims=True)
    inv = lax.rsqrt(jnp.mean(cen * cen, -1, keepdims=True) + NORM_EPS)
    normed = cen * inv
    ee = e[...].astype(F32)
    ig[...] = og[...] + inv * (
        ee - jnp.mean(ee, -1, keepdims=True) - normed * jnp.mean(ee * normed, -1, keepdims=True)
    )

    def summed(slots, p):
        total = slots[p].astype(F32)
        for j in range(1, d.nc // 2):
            total += slots[2 * j + p].astype(F32)
        return total

    @pl.when(pl.program_id(0) == 0)
    def _():
        for p in range(2):
            rows = slice(p * HR, (p + 1) * HR)
            half_a = summed(fa, p)
            for j in range(3):
                o_qkv[j, rows, :] = half_a[:, j * hs : (j + 1) * hs]
            o_fc1[rows, :] = summed(fb, p)
            o_fc2[rows, :] = summed(fc, p)
        whole_a = jnp.concatenate([summed(fa, 0), summed(fa, 1)], 0)
        o_wo[...] = jnp.transpose(whole_a[:, 3 * hs :])
        for k, (o, n) in enumerate(
            ((o_g1, D), (o_b1, D), (o_g2, D), (o_b2, D), (o_bo, D), (o_bf1, F))
        ):
            o[...] = small[k : k + 1, :n].reshape(n)
        o_bf2[...] = small[4:5, :D].reshape(D)
        for j in range(3):
            o_bqkv[j : j + 1, :] = small[6:7, j * hs : (j + 1) * hs]


def solution(mesh):
    in_specs = (
        P(("fsdp", "ctx"), None),
        P("fsdp"),
        P(("fsdp", "ctx")),
        P(),
        P(),
        P(),
        P(),
        P("fsdp", None, "tp"),
        P(None, "tp"),
        P("tp", "fsdp"),
        P(),
        P("fsdp", "tp"),
        P("tp"),
        P("tp", "fsdp"),
        P(),
        P(("fsdp", "ctx"), None),
    )
    out_specs = (
        P(("fsdp", "ctx"), None),
        P(("fsdp", "ctx"), None),
        P(),
        P(),
        P(),
        P(),
        P("fsdp", None, "tp"),
        P(None, "tp"),
        P("tp", "fsdp"),
        P(),
        P("fsdp", "tp"),
        P("tp"),
        P("tp", "fsdp"),
        P(),
    )

    def step(*args):
        return body(mesh, *args)

    return jax.shard_map(step, mesh=mesh, in_specs=in_specs, out_specs=out_specs, check_vma=False)
```

```python
import math

import jax
import jax.numpy as jnp
from jax import lax
from jax.experimental import pallas as pl
from jax.experimental.pallas import tpu as pltpu
from jax.sharding import PartitionSpec as P

HD = 64
ROT = 16
HALF = ROT // 2
NEG_FILL = -1e30
NORM_EPS = 1e-05
INV_ROOT_TWO = 0.7071067811865476
INV_ROOT_TWO_PI = 0.3989422804014327
F32 = jnp.float32
BF16 = jnp.bfloat16
VMEM_BYTES = 67043328


def mm(a, b):
    return jnp.dot(a, b, preferred_element_type=F32)


def mm_nt(a, b):
    return lax.dot_general(a, b, (((1,), (1,)), ((), ())), preferred_element_type=F32)


def tile_rows(i, size):
    return pl.ds(pl.multiple_of(i * size, size), size)


class Dims:
    def __init__(self, mesh, tokens, width, span, hidden):
        self.nz, self.nc, self.nt = mesh.shape["fsdp"], mesh.shape["ctx"], mesh.shape["tp"]
        self.tok, self.width, self.span, self.hidden = tokens, width, span, hidden
        self.heads = span // HD
        self.blk = min(512, tokens)
        self.nb = tokens // self.blk
        self.nkb = self.nc * self.nb
        self.tail = (3 * self.nkb) // 4
        self.rows = width // self.nz
        self.half = self.rows // 2
        self.tile = min(256, tokens)
        self.nx = self.nt // 2
        self.keep = self.nc <= 2
        assert 4 * span == hidden and self.nt % 2 == 0 and self.nc % 2 == 0
        self.wide = max(width, hidden, 3 * span)
        nz, nc, nx = self.nz, self.nc, self.nx
        self.n_copies = (
            3 * 4 * (nz - 1)
            + 2 * (nc - 1)
            + 2 * (nx + 1)
            + 2 * (nz + (nz - 1) + (nc - 1))
            + (nz - 1)
            + (nc - 1)
            + (nz * nc - 1)
            + (self.nt - 1)
        )


class Net:
    def __init__(self, send, recv):
        self.send, self.recv, self.used, self.started = send, recv, 0, []

    def copy(self, src, dst, device):
        i = self.used
        self.used += 1
        return pltpu.make_async_remote_copy(
            src_ref=src,
            dst_ref=dst,
            send_sem=self.send.at[i],
            recv_sem=self.recv.at[i],
            device_id=device,
            device_id_type=pl.DeviceIdType.MESH,
        )


def layer_kernel(d, *refs):
    (x, og, pos_in, gain1, shift1, gain2, shift2, bq_in, bf_in, wq_in, wo_in, wb, wc) = refs[:13]
    (u_out, e_out, ga_out, gb_out, gc_out, sm_out) = refs[13:19]
    (
        WA, WB, WC, WT, h1, h2, tA, gb, gbT, mean_s, inv_s, act, dpre,
        qz, kv, kvn, doz, ctxT, lse, dlt, dq, dkv,
        ra, chU, chE, finU, finE,
        ggA, ggB, ggC, r1A, r1B, r2A, r2B, r2C, f3A, f3B, f3C,
        sm, smr, smt, out, ig, wa, cosr, sinr, pos, send, recv, local,
    ) = refs[19:]
    ub = h2
    if not d.keep:
        ggA = ggB
    T, D, hs, F = d.tok, d.width, d.span, d.hidden
    nz, nc, nt, nx = d.nz, d.nc, d.nt, d.nx
    heads, B, nb, R, HR, TB = d.heads, d.blk, d.nb, d.rows, d.half, d.tile
    z, c, t = lax.axis_index("fsdp"), lax.axis_index("ctx"), lax.axis_index("tp")
    part = lax.rem(c, 2)
    other = 1 - part
    pair = c + 1 - 2 * part
    core = lax.rem(t, 2)
    xg = t // 2
    mate = t + 1 - 2 * core
    net = Net(send, recv)
    scale = HD ** (-0.5)

    def turn(value, step, size):
        return lax.rem(value + step, size)

    barrier = pltpu.get_barrier_semaphore()
    talks = []
    for rz in range(nz):
        for rc in range(nc):
            if rz or rc:
                talks.append((turn(z, rz, nz), turn(c, rc, nc), t))
    for rt in range(1, nt):
        talks.append((z, c, turn(t, rt, nt)))
    for device in talks:
        pl.semaphore_signal(barrier, inc=1, device_id=device, device_id_type=pl.DeviceIdType.MESH)
    pl.semaphore_wait(barrier, len(talks))

    half_here = pl.ds(pl.multiple_of(part * HR, HR), HR)

    def rows_of(src):
        return pl.ds(pl.multiple_of(src * R + part * HR, HR), HR)

    wa[...] = jnp.concatenate([wq_in[0], wq_in[1], wq_in[2], jnp.transpose(wo_in[...])], 1)

    class Gather:
        def __init__(self, shard, full):
            self.moves = []
            for step in (1, -1):
                to = jnp.clip(z + step, 0, nz - 1)
                has_next = (z + 1 < nz) if step == 1 else (z > 0)
                for k in range(1, nz):
                    sent, come = z - step * (k - 1), z - step * k
                    inside = (come >= 0) if step == 1 else (come < nz)
                    has_sent = (sent >= 0) if step == 1 else (sent < nz)
                    at = rows_of(jnp.clip(sent, 0, nz - 1))
                    src = shard.at[half_here] if k == 1 else full.at[at]
                    hop = net.copy(src, full.at[at], (to, c, t))
                    got = rows_of(jnp.clip(come, 0, nz - 1))
                    side = net.copy(full.at[got], full.at[got], (z, pair, t))
                    self.moves.append((k, hop, side, inside, has_next, has_sent & has_next))

        def start(self):
            for k, hop, side, inside, has_next, sends in self.moves:
                if k == 1:
                    pl.when(sends)(hop.start)

        def pump(self, k):
            for i, (kk, hop, side, inside, has_next, sends) in enumerate(self.moves):
                if kk == k:
                    onward = self.moves[i + 1] if k + 1 < nz else None

                    @pl.when(inside)
                    def _():
                        hop.wait_recv()
                        if onward is not None:
                            pl.when(has_next)(onward[1].start)
                        side.start()

        def done(self):
            for k, hop, side, inside, has_next, sends in self.moves:
                pl.when(inside)(side.wait_recv)

        def drain(self):
            for k, hop, side, inside, has_next, sends in self.moves:
                pl.when(sends)(hop.wait_send)
                pl.when(inside)(side.wait_send)

    gather_a, gather_b, gather_c = [
        Gather(shard, full) for shard, full in ((wa, WA), (wb, WB), (wc, WC))
    ]
    gather_a.start()

    sm[...] = jnp.zeros_like(sm)
    g1, b1, g2, b2 = [one[...].reshape(1, D) for one in (gain1, shift1, gain2, shift2)]
    bf1 = bf_in[...].reshape(1, F)
    positions = pos_in[...].reshape(1, T)
    exponent = lax.broadcasted_iota(jnp.int32, (HALF, 1), 0).astype(F32) * (-2.0 / ROT)
    freqs = jnp.exp(exponent * math.log(10000.0))
    for i in range(nb):
        pos[i] = positions[:, i * B : (i + 1) * B]
        angle = pos[i].astype(F32) * freqs
        cosr[i] = jnp.cos(angle)
        sinr[i] = jnp.sin(angle)
    bq = jnp.concatenate(
        [jnp.transpose(jnp.broadcast_to(bq_in[j : j + 1, :], (128, hs)))[:, :1] for j in range(3)], 0
    )

    def norm_tile(i, carry):
        rows = tile_rows(i, TB)
        xf = x[rows, :].astype(F32)
        mean = jnp.mean(xf, -1, keepdims=True)
        cen = xf - mean
        inv = lax.rsqrt(jnp.mean(cen * cen, -1, keepdims=True) + NORM_EPS)
        normed = cen * inv
        mean_s[rows, :] = mean
        inv_s[rows, :] = inv
        h1[rows, :] = (normed * g1 + b1).astype(BF16)
        h2[rows, :] = (normed * g2 + b2).astype(BF16)
        grad = og[rows, :]
        gb[rows, :] = grad.astype(BF16)
        sm[4:5, :D] += jnp.sum(grad, 0, keepdims=True)
        return carry

    lax.fori_loop(0, T // TB, norm_tile, 0)
    own_rows = pl.ds(pl.multiple_of(z * R, R), R)
    WA[own_rows, :] = wa[...]
    WB[own_rows, :] = wb[...]
    WC[own_rows, :] = wc[...]
    for i in range(nb):
        gbT[i] = jnp.transpose(gb[i * B : (i + 1) * B, :])
        tA[:, i * B : (i + 1) * B] = jnp.transpose(h2[i * B : (i + 1) * B, :])

    for k in range(1, nz):
        gather_a.pump(k)
        if k == max(1, nz - 2):
            gather_b.start()
    gather_a.done()
    WT[...] = jnp.transpose(WA[...])
    gather_b.pump(1)

    for i in range(nb):
        proj = mm_nt(WT[: 3 * hs, :], h1[i * B : (i + 1) * B, :]) + bq
        cb, sb = cosr[i], sinr[i]

        def rotated(tensor):
            lo, hi = tensor[:HALF], tensor[HALF:ROT]
            return jnp.concatenate([lo * cb - hi * sb, hi * cb + lo * sb, tensor[ROT:]], 0)

        own = c * nb + i
        for h in range(heads):
            q = rotated(proj[h * HD : (h + 1) * HD]).astype(BF16) * jnp.asarray(scale, BF16)
            qz[i, h] = jnp.concatenate([q, jnp.zeros_like(q)], 0)
            key = rotated(proj[hs + h * HD : hs + (h + 1) * HD]).astype(BF16)
            value = proj[2 * hs + h * HD : 2 * hs + (h + 1) * HD].astype(BF16)
            both = jnp.concatenate([key, value], 0)
            kv[own, h] = both
            if d.keep:
                kvn[own, h] = jnp.transpose(both)

    for k in range(2, nz):
        gather_b.pump(k)
        if k == max(2, nz - 2):
            gather_c.start()
    own_blocks = pl.ds(c * nb, nb)
    kv_out = [
        net.copy(kv.at[own_blocks], kv.at[own_blocks], (z, turn(c, r, nc), t))
        for r in range(1, nc)
    ]
    gather_c.pump(1)

    for i in range(nb):
        dct = mm(WT[3 * hs :, :], gbT[i]).astype(BF16)
        for h in range(heads):
            piece = dct[h * HD : (h + 1) * HD]
            doz[i, h] = jnp.concatenate([jnp.zeros_like(piece), piece], 0)

    for k in range(2, nz):
        gather_c.pump(k)
    for r, one in enumerate(kv_out, 1):

        @pl.when(c + r < nc)
        def _(one=one):
            one.start()

    gather_b.done()
    gather_c.done()

    def normed_of(rows):
        return (x[rows, :].astype(F32) - mean_s[rows, :]) * inv_s[rows, :]

    def mlp_tile(i, carry):
        rows = tile_rows(i, TB)
        pre = mm(h2[rows, :], WB[...]) + bf1
        cdf = 0.5 * (1.0 + lax.erf(pre * INV_ROOT_TWO))
        density = jnp.exp(-0.5 * pre * pre) * INV_ROOT_TWO_PI
        actb = (pre * cdf).astype(BF16)
        act[rows, :] = actb
        dp = mm(gb[rows, :], WC[...]) * (cdf + pre * density)
        sm[5:6, :F] += jnp.sum(dp, 0, keepdims=True)
        dpb = dp.astype(BF16)
        dpre[rows, :] = dpb
        out[rows, :] = mm_nt(actb, WC[...])
        dh2 = mm_nt(dpb, WB[...])
        sm[2:3, :D] += jnp.sum(dh2 * normed_of(rows), 0, keepdims=True)
        sm[3:4, :D] += jnp.sum(dh2, 0, keepdims=True)
        ig[rows, :] = dh2 * g2
        return carry

    lax.fori_loop(0, T // TB, mlp_tile, 0)

    def store_grad(gg, value, z0):
        for k in range(value.shape[0] // HR):
            gg[k % 2, z0 + k // 2] = value[k * HR : (k + 1) * HR].astype(BF16)

    class Reduce:
        def __init__(self, i, gg, r1, r2, f3, final):
            self.gg, self.r1, self.r2, self.f3 = gg, r1, r2, f3
            self.put = pltpu.make_async_copy(f3, final, local.at[i])
            self.a = [
                net.copy(gg.at[other, turn(z, r, nz)], r1.at[turn(z, r, nz)], (z, pair, t))
                for r in range(nz)
            ]
            self.b = [
                net.copy(gg.at[part, turn(z, r, nz)], r2.at[r - 1], (turn(z, r, nz), c, t))
                for r in range(1, nz)
            ]
            self.c = [net.copy(f3.at[c], f3.at[c], (z, turn(c, r, nc), t)) for r in range(1, nc)]

        def one(self):
            for one in [*self.a[1:], self.a[0]]:
                one.start()

        def two(self):
            for r in range(1, nz):
                self.a[r].wait_recv()
                zz = turn(z, r, nz)
                self.gg[part, zz] = (self.gg[part, zz].astype(F32) + self.r1[zz].astype(F32)).astype(BF16)
                self.b[r - 1].start()

        def three(self):
            self.a[0].wait_recv()
            total = self.gg[part, z].astype(F32) + self.r1[z].astype(F32)
            for r in range(1, nz):
                self.b[r - 1].wait_recv()
                total += self.r2[r - 1].astype(F32)
            self.f3[c] = total.astype(BF16)
            for one in self.c:
                one.start()

        def four(self):
            for one in self.c:
                one.wait_recv()
            self.put.start()

        def drain(self):
            for one in [*self.a, *self.b, *self.c]:
                one.wait_send()

    class ReduceFlat:
        def __init__(self, i, gg, r2, f3, final):
            self.gg, self.r2, self.f3 = gg, r2, f3
            self.put = pltpu.make_async_copy(f3, final, local.at[i])
            self.b = [
                net.copy(gg.at[turn(z, r, nz)], r2.at[r - 1], (turn(z, r, nz), c, t))
                for r in range(1, nz)
            ]
            self.c = [net.copy(f3.at[c], f3.at[c], (z, turn(c, r, nc), t)) for r in range(1, nc)]

        def one(self):
            for one in self.b:
                one.start()

        def three(self):
            total = self.gg[z].astype(F32)
            for r in range(1, nz):
                self.b[r - 1].wait_recv()
                total += self.r2[r - 1].astype(F32)
            self.f3[c] = total.astype(BF16)
            for one in self.c:
                one.start()

        def four(self):
            for one in self.c:
                one.wait_recv()
            self.put.start()

        def drain(self):
            for one in [*self.b, *self.c]:
                one.wait_send()

    redB = Reduce(0, ggB, r1B, r2B, f3B, gb_out)
    redC = ReduceFlat(1, ggC, r2C, f3C, gc_out)
    redA = Reduce(2, ggA, r1A, r2A, f3A, ga_out)

    for z0 in range(0, nz, 2):
        store_grad(ggB, mm(tA[z0 * R : (z0 + 2) * R, :], dpre[...]), z0)
    redB.one()
    for z0 in range(0, nz, 2):
        value = None
        for i in range(nb):
            term = mm(gbT[i, z0 * R : (z0 + 2) * R, :], act[i * B : (i + 1) * B, :])
            value = term if value is None else value + term
        for k in range(2):
            ggC[z0 + k] = value[k * R : (k + 1) * R].astype(BF16)
    redC.one()

    for r, one in enumerate(kv_out, 1):

        @pl.when(c >= r)
        def _(r=r, one=one):
            one.wait_recv()

            def flip(j, carry):
                at = (c - r) * nb + j
                for h in range(heads):
                    kvn[at, h] = jnp.transpose(kv[at, h])
                return carry

            if d.keep:
                lax.fori_loop(0, nb, flip, 0)

    def natural(at, h):
        return kvn[at, h] if d.keep else jnp.transpose(kv[at, h])

    def allowed_of(i, at):
        query_at = (c * nb + i) * B + lax.broadcasted_iota(jnp.int32, (1, B), 1)
        key_at = at * B + lax.broadcasted_iota(jnp.int32, (B, 1), 0)
        return (key_at <= query_at) & (key_at >= query_at - pos[i])

    for i in range(nb):
        here = c * nb + i
        first_key = jnp.where(here >= d.tail, d.tail, 0)
        for h in range(heads):
            qh = qz[i, h]

            def key_step(at, carry, i=i, h=h, qh=qh):
                top, total, weighted = carry
                s = jnp.where(allowed_of(i, at), mm(natural(at, h), qh), NEG_FILL)
                new_top = jnp.maximum(top, jnp.max(s, 0, keepdims=True))
                w = jnp.exp(s - new_top)
                factor = jnp.exp(top - new_top)
                total = total * factor + jnp.sum(w, 0, keepdims=True)
                weighted = weighted * factor + mm(kv[at, h, HD:], w.astype(BF16))
                return new_top, total, weighted

            top, total, weighted = lax.fori_loop(
                first_key,
                here + 1,
                key_step,
                (
                    jnp.full((1, B), NEG_FILL, F32),
                    jnp.zeros((1, B), F32),
                    jnp.zeros((HD, B), F32),
                ),
            )
            lse[i, h : h + 1, :] = top + jnp.log(total)
            ctx_h = (weighted / total).astype(BF16)
            ctxT[i, h * HD : (h + 1) * HD, :] = ctx_h
            dlt[i, h : h + 1, :] = jnp.sum(
                doz[i, h, HD:].astype(F32) * ctx_h.astype(F32), 0, keepdims=True
            )

    class Join:
        def __init__(self, ra, ch, fin):
            self.ra, self.ch, self.fin = ra, ch, fin
            self.near = net.copy(
                ub.at[pl.ds(pl.multiple_of((1 - core) * (T // 2), T // 2), T // 2)], ra, (z, c, mate)
            )
            self.far = [
                net.copy(ch.at[xg], ch.at[xg], (z, c, turn(xg, r, nx) * 2 + core))
                for r in range(1, nx)
            ]
            self.back = net.copy(fin.at[core], fin.at[core], (z, c, mate))

        def one(self):
            self.near.start()

        def two(self):
            self.near.wait_recv()
            for k in range(T // 2 // TB):
                mine = pl.ds(pl.multiple_of(core * (T // 2) + k * TB, TB), TB)
                tile = slice(k * TB, (k + 1) * TB)
                self.ch[xg, tile, :] = (
                    ub[mine, :].astype(F32) + self.ra[tile, :].astype(F32)
                ).astype(BF16)
            for one in self.far:
                one.start()

        def three(self):
            for one in self.far:
                one.wait_recv()
            for k in range(T // 2 // TB):
                tile = slice(k * TB, (k + 1) * TB)
                total = self.ch[0, tile, :].astype(F32)
                for j in range(1, nx):
                    total += self.ch[j, tile, :].astype(F32)
                self.fin[core, tile, :] = total.astype(BF16)
            self.back.start()

        def four(self):
            self.back.wait_recv()

        def drain(self):
            for one in [*self.far, self.back]:
                one.wait_send()

    join_u = Join(ra, chU, finU)
    join_e = Join(ra, chE, finE)

    for i in range(nb):
        ctx_n = jnp.transpose(ctxT[i])
        for k in range(B // TB):
            rows = slice(i * B + k * TB, i * B + (k + 1) * TB)
            ub[rows, :] = (
                out[rows, :] + mm(ctx_n[k * TB : (k + 1) * TB], WT[3 * hs :, :])
            ).astype(BF16)
    join_u.one()

    dq[...] = jnp.zeros_like(dq)

    def key_back(at, h, put):
        k_t = kv[at, h, :HD]
        k_n = natural(at, h)

        def query_step(i, carry):
            dk, dv = carry
            s = mm(k_n, qz[i, h])
            ok = allowed_of(i, at)
            prob = jnp.where(ok, jnp.exp(s - lse[i, h : h + 1, :]), 0.0)
            dp = mm(k_n, doz[i, h])
            ds = (prob * (dp - dlt[i, h : h + 1, :])).astype(BF16)
            dv = dv + mm_nt(doz[i, h, HD:], prob.astype(BF16))
            dk = dk + mm_nt(qz[i, h, :HD], ds)
            dq[i, h] += mm(k_t, ds)
            return dk, dv

        begin = jnp.maximum(at - c * nb, 0)
        end = jnp.where(at < d.tail, jnp.minimum(nb, d.tail - c * nb), nb)
        zero = jnp.zeros((HD, B), F32)
        put(lax.fori_loop(begin, end, query_step, (zero, zero)))

    dkv_out = []
    for r in range(1, nc):
        owner = turn(c, nc - r, nc)
        dkv_out.append(net.copy(kv.at[pl.ds(owner * nb, nb)], kv.at[own_blocks], (z, owner, t)))
    for r in reversed(range(1, nc)):

        @pl.when(c >= r)
        def _(r=r):
            def block(j, carry):
                for h in range(heads):

                    def put(pieces, h=h):
                        kv[(c - r) * nb + j, h, :HD] = pieces[0].astype(BF16)
                        kv[(c - r) * nb + j, h, HD:] = pieces[1].astype(BF16)

                    key_back((c - r) * nb + j, h, put)
                return carry

            lax.fori_loop(0, nb, block, 0)
            dkv_out[r - 1].start()

    join_u.two()

    def own_block(j, carry):
        for h in range(heads):

            def put(pieces, h=h):
                dkv[j, h, :HD] = pieces[0]
                dkv[j, h, HD:] = pieces[1]

            key_back(c * nb + j, h, put)
        return carry

    lax.fori_loop(0, nb, own_block, 0)
    redB.two()
    join_u.three()

    for r in range(1, nc):

        @pl.when(c + r < nc)
        def _(r=r):
            dkv_out[r - 1].wait_recv()
            for j in range(nb):
                for h in range(heads):
                    dkv[j, h] += kv[(c + r) * nb + j, h].astype(F32)

    grad_t = None
    bias_t = jnp.zeros((3 * hs, 1), F32)
    for i in range(nb):
        cb, sb = cosr[i], sinr[i]

        def unrotated(g):
            lo, hi = g[:HALF], g[HALF:ROT]
            return jnp.concatenate([lo * cb + hi * sb, hi * cb - lo * sb, g[ROT:]], 0)

        pieces = [unrotated(dq[i, h] * scale) for h in range(heads)]
        pieces += [unrotated(dkv[i, h, :HD]) for h in range(heads)]
        pieces += [dkv[i, h, HD:] for h in range(heads)]
        d_proj = jnp.concatenate(pieces, 0)
        bias_t += jnp.sum(d_proj, -1, keepdims=True)
        d_proj_b = d_proj.astype(BF16)
        tA[: 3 * hs, i * B : (i + 1) * B] = d_proj_b
        act[i * B : (i + 1) * B, : 3 * hs] = jnp.transpose(d_proj_b)
    sm[6:7, : 3 * hs] = jnp.transpose(jnp.broadcast_to(bias_t, (3 * hs, 128)))[0:1, :]

    grad_q = mm(tA[: 3 * hs, :], h1[...])
    grad_o = None
    for i in range(nb):
        term = mm(ctxT[i], gb[i * B : (i + 1) * B, :])
        grad_o = term if grad_o is None else grad_o + term
    grad_a = jnp.transpose(jnp.concatenate([grad_q.astype(BF16), grad_o.astype(BF16)], 0))
    if not d.keep:
        for one in [*redB.a, *redB.b]:
            one.wait_send()
    store_grad(ggA, grad_a, 0)
    redA.one()
    join_u.near.wait_send()

    def e_tile(i, carry):
        rows = tile_rows(i, TB)
        dh1 = mm(act[rows, : 3 * hs], WT[: 3 * hs, :])
        sm[0:1, :D] += jnp.sum(dh1 * normed_of(rows), 0, keepdims=True)
        sm[1:2, :D] += jnp.sum(dh1, 0, keepdims=True)
        ub[rows, :] = (ig[rows, :] + dh1 * g1).astype(BF16)
        return carry

    lax.fori_loop(0, T // TB, e_tile, 0)
    join_u.four()
    join_e.one()
    redC.three()

    rank = z * nc + c
    smr[rank] = sm[...]
    small_a = []
    for rz in range(nz):
        for rc in range(nc):
            if rz or rc:
                small_a.append(
                    net.copy(smr.at[rank], smr.at[rank], (turn(z, rz, nz), turn(c, rc, nc), t))
                )
    for one in small_a:
        one.start()
    join_e.two()
    redB.three()
    redA.two()

    put_u = pltpu.make_async_copy(finU, u_out, local.at[3])
    put_u.start()
    redB.four()
    redC.four()

    for one in small_a:
        one.wait_recv()
    tot = smr[0]
    for j in range(1, nz * nc):
        tot += smr[j]
    smt[t] = tot
    small_b = [net.copy(smt.at[t], smt.at[t], (z, c, turn(t, r, nt))) for r in range(1, nt)]
    for one in small_b:
        one.start()
    redA.three()
    join_e.three()
    for one in small_b:
        one.wait_recv()
    tops = smt[0, 0:4, :]
    for j in range(1, nt):
        tops += smt[j, 0:4, :]
    sm_out[...] = jnp.concatenate([tops, tot[4:8, :]], 0)
    join_e.four()

    put_e = pltpu.make_async_copy(finE, e_out, local.at[4])
    put_e.start()
    redA.four()

    for one in (gather_a, gather_b, gather_c):
        one.drain()
    for r, one in enumerate(kv_out, 1):

        @pl.when(c + r < nc)
        def _(one=one):
            one.wait_send()

    for r, one in enumerate(dkv_out, 1):

        @pl.when(c >= r)
        def _(one=one):
            one.wait_send()

    for one in redB.c if not d.keep else [*redB.a, *redB.b, *redB.c]:
        one.wait_send()
    redA.drain()
    redC.drain()
    join_u.drain()
    join_e.near.wait_send()
    join_e.drain()
    for one in [*small_a, *small_b]:
        one.wait_send()
    for one in (redA.put, redB.put, redC.put, put_u, put_e):
        one.wait()
    assert net.used == d.n_copies


def body(
    mesh,
    layer_input,
    segments,
    positions,
    ln1_gain,
    ln1_bias,
    ln2_gain,
    ln2_bias,
    w_qkv,
    b_qkv,
    w_out,
    b_out,
    w_fc1,
    b_fc1,
    w_fc2,
    b_fc2,
    out_grad,
):
    d = Dims(mesh, layer_input.shape[0], layer_input.shape[1], b_qkv.shape[1], b_fc1.shape[0])
    T, D, hs, F, B, nb = d.tok, d.width, d.span, d.hidden, d.blk, d.nb
    R, HR, nz, nc = d.rows, d.half, d.nz, d.nc
    wide_a = 4 * hs
    args = (
        layer_input,
        out_grad,
        positions,
        ln1_gain,
        ln1_bias,
        ln2_gain,
        ln2_bias,
        b_qkv,
        b_fc1,
        jnp.transpose(w_qkv, (1, 0, 2)),
        w_out,
        w_fc1,
        w_fc2.T,
    )
    vm = pltpu.VMEM
    h, W = d.heads, d.wide
    scratch = [
        vm((D, wide_a), BF16), vm((D, F), BF16), vm((D, F), BF16), vm((wide_a, D), BF16),
        vm((T, D), BF16), vm((T, D), BF16), vm((D, T), BF16), vm((T, D), BF16), vm((nb, D, B), BF16),
        vm((T, 1), F32), vm((T, 1), F32), vm((T, F), BF16), vm((T, F), BF16),
        vm((nb, h, 2 * HD, B), BF16), vm((d.nkb, h, 2 * HD, B), BF16), vm((d.nkb if d.keep else 1, h, B, 2 * HD), BF16),
        vm((nb, h, 2 * HD, B), BF16), vm((nb, hs, B), BF16),
        vm((nb, 8, B), F32), vm((nb, 8, B), F32), vm((nb, h, HD, B), F32),
        vm((nb, h, 2 * HD, B), F32),
        vm((T // 2, D), BF16),
        vm((d.nx, T // 2, D), BF16), vm((d.nx, T // 2, D), BF16),
        vm((2, T // 2, D), BF16), vm((2, T // 2, D), BF16),
    ]
    widths = (wide_a, F, F)
    piece = (HR, HR, R)
    scratch += [vm((2, nz, HR, wide_a) if d.keep else (8, 128), BF16)]
    scratch += [vm((2, nz, HR, F), BF16), vm((nz, R, F), BF16)]
    scratch += [vm((nz, HR, w), BF16) for w in widths[:2]]
    scratch += [vm((nz - 1, n, w), BF16) for n, w in zip(piece, widths)]
    scratch += [vm((nc, n, w), BF16) for n, w in zip(piece, widths)]
    scratch += [vm((8, W), F32), vm((nz * nc, 8, W), F32), vm((d.nt, 8, W), F32)]
    scratch += [vm((T, D), F32), vm((T, D), F32), vm((R, wide_a), BF16)]
    scratch += [vm((nb, HALF, B), F32), vm((nb, HALF, B), F32), vm((nb, 1, B), jnp.int32)]
    scratch += [pltpu.SemaphoreType.DMA((n,)) for n in (d.n_copies, d.n_copies, 5)]

    def kernel(*refs):
        layer_kernel(d, *refs)

    fin = jax.ShapeDtypeStruct((2, T // 2, D), BF16)
    sums = [jax.ShapeDtypeStruct((nc, n, w), BF16) for n, w in zip(piece, widths)]
    in_hbm = pl.BlockSpec(memory_space=pl.ANY)
    joined, joined_e, *owned, small = pl.pallas_call(
        kernel,
        out_shape=(fin, fin, *sums, jax.ShapeDtypeStruct((8, W), F32)),
        in_specs=[pl.BlockSpec(memory_space=vm)] * len(args),
        out_specs=[in_hbm] * 5 + [pl.BlockSpec(memory_space=vm)],
        scratch_shapes=scratch,
        compiler_params=pltpu.CompilerParams(
            collective_id=0, has_side_effects=True, vmem_limit_bytes=VMEM_BYTES
        ),
    )(*args)

    TB = d.tile

    def tiles():
        return pl.BlockSpec((TB, D), lambda i: (i, 0))

    def whole(shape):
        return pl.BlockSpec(shape, lambda i: (0,) * len(shape))

    outs = [
        ((T, D), True), ((T, D), True), ((D,), False), ((D,), False), ((D,), False), ((D,), False),
        ((3, R, hs), False), ((3, hs), False), ((hs, R), False), ((D,), False), ((R, F), False),
        ((F,), False), ((R, F), False), ((D,), False),
    ]
    results = pl.pallas_call(
        lambda *refs: finish_kernel(d, *refs),
        grid=(T // TB,),
        out_shape=[jax.ShapeDtypeStruct(shape, F32) for shape, _ in outs],
        in_specs=[tiles(), tiles(), tiles(), tiles()]
        + [whole(o.shape) for o in owned]
        + [whole((8, W)), whole((D,)), whole((D,))],
        out_specs=[tiles() if tiled else whole(shape) for shape, tiled in outs],
        compiler_params=pltpu.CompilerParams(vmem_limit_bytes=VMEM_BYTES),
    )(
        layer_input, out_grad, joined.reshape(T, D), joined_e.reshape(T, D), *owned, small, b_out, b_fc2
    )
    results = list(results)
    results[6] = jnp.transpose(results[6], (1, 0, 2))
    results[12] = results[12].T
    return tuple(results)


def finish_kernel(d, x, og, u, e, fa, fb, fc, small, bo, bf2, *outs):
    out, ig, o_g1, o_b1, o_g2, o_b2, o_qkv, o_bqkv, o_wo, o_bo, o_fc1, o_bf1, o_fc2, o_bf2 = outs
    D, hs, F, HR = d.width, d.span, d.hidden, d.half
    xf = x[...].astype(F32)
    out[...] = xf + u[...].astype(F32) + (bo[...] + bf2[...]).reshape(1, D)
    cen = xf - jnp.mean(xf, -1, keepdims=True)
    inv = lax.rsqrt(jnp.mean(cen * cen, -1, keepdims=True) + NORM_EPS)
    normed = cen * inv
    ee = e[...].astype(F32)
    ig[...] = og[...] + inv * (
        ee - jnp.mean(ee, -1, keepdims=True) - normed * jnp.mean(ee * normed, -1, keepdims=True)
    )

    def summed(slots, p):
        total = slots[p].astype(F32)
        for j in range(1, d.nc // 2):
            total += slots[2 * j + p].astype(F32)
        return total

    @pl.when(pl.program_id(0) == 0)
    def _():
        for p in range(2):
            rows = slice(p * HR, (p + 1) * HR)
            half_a = summed(fa, p)
            for j in range(3):
                o_qkv[j, rows, :] = half_a[:, j * hs : (j + 1) * hs]
            o_fc1[rows, :] = summed(fb, p)
        total = fc[0].astype(F32)
        for j in range(1, d.nc):
            total += fc[j].astype(F32)
        o_fc2[...] = total
        whole_a = jnp.concatenate([summed(fa, 0), summed(fa, 1)], 0)
        o_wo[...] = jnp.transpose(whole_a[:, 3 * hs :])
        for k, (o, n) in enumerate(
            ((o_g1, D), (o_b1, D), (o_g2, D), (o_b2, D), (o_bo, D), (o_bf1, F))
        ):
            o[...] = small[k : k + 1, :n].reshape(n)
        o_bf2[...] = small[4:5, :D].reshape(D)
        for j in range(3):
            o_bqkv[j : j + 1, :] = small[6:7, j * hs : (j + 1) * hs]


def solution(mesh):
    in_specs = (
        P(("fsdp", "ctx"), None),
        P("fsdp"),
        P(("fsdp", "ctx")),
        P(),
        P(),
        P(),
        P(),
        P("fsdp", None, "tp"),
        P(None, "tp"),
        P("tp", "fsdp"),
        P(),
        P("fsdp", "tp"),
        P("tp"),
        P("tp", "fsdp"),
        P(),
        P(("fsdp", "ctx"), None),
    )
    out_specs = (
        P(("fsdp", "ctx"), None),
        P(("fsdp", "ctx"), None),
        P(),
        P(),
        P(),
        P(),
        P("fsdp", None, "tp"),
        P(None, "tp"),
        P("tp", "fsdp"),
        P(),
        P("fsdp", "tp"),
        P("tp"),
        P("tp", "fsdp"),
        P(),
    )

    def step(*args):
        return body(mesh, *args)

    return jax.shard_map(step, mesh=mesh, in_specs=in_specs, out_specs=out_specs, check_vma=False)
```

```python
import math

import jax
import jax.numpy as jnp
from jax import lax
from jax.experimental import pallas as pl
from jax.experimental.pallas import tpu as pltpu
from jax.sharding import PartitionSpec as P

HD = 64
ROT = 16
HALF = ROT // 2
NEG_FILL = -1e30
NORM_EPS = 1e-05
INV_ROOT_TWO = 0.7071067811865476
INV_ROOT_TWO_PI = 0.3989422804014327
F32 = jnp.float32
BF16 = jnp.bfloat16
VMEM_BYTES = 67043328


def mm(a, b):
    return jnp.dot(a, b, preferred_element_type=F32)


def mm_nt(a, b):
    return lax.dot_general(a, b, (((1,), (1,)), ((), ())), preferred_element_type=F32)


def tile_rows(i, size):
    return pl.ds(pl.multiple_of(i * size, size), size)


class Dims:
    def __init__(self, mesh, tokens, width, span, hidden):
        self.nz, self.nc, self.nt = mesh.shape["fsdp"], mesh.shape["ctx"], mesh.shape["tp"]
        self.tok, self.width, self.span, self.hidden = tokens, width, span, hidden
        self.heads = span // HD
        self.blk = min(512, tokens)
        self.nb = tokens // self.blk
        self.nkb = self.nc * self.nb
        self.tail = (3 * self.nkb) // 4
        self.rows = width // self.nz
        self.half = self.rows // 2
        self.tile = min(256, tokens)
        self.nx = self.nt // 2
        self.keep = self.nc <= 2
        assert 4 * span == hidden and self.nt % 2 == 0 and self.nc % 2 == 0
        self.wide = max(width, hidden, 3 * span)
        nz, nc, nx = self.nz, self.nc, self.nx
        self.n_copies = (
            3 * 4 * (nz - 1)
            + (nc - 1) * (1 + self.nb)
            + 2 * 2 * (nx + 1)
            + 3 * (nz + (nz - 1) + (nc - 1))
            + (nz - 1)
            + (nc - 1)
            + (nz * nc - 1)
            + (self.nt - 1)
        )


class Net:
    def __init__(self, send, recv):
        self.send, self.recv, self.used, self.started = send, recv, 0, []

    def copy(self, src, dst, device):
        i = self.used
        self.used += 1
        return pltpu.make_async_remote_copy(
            src_ref=src,
            dst_ref=dst,
            send_sem=self.send.at[i],
            recv_sem=self.recv.at[i],
            device_id=device,
            device_id_type=pl.DeviceIdType.MESH,
        )


def layer_kernel(d, *refs):
    (x_in, og_in, pos_in, gain1, shift1, gain2, shift2, bq_in, bf_in, wq_in, wo_in, wb, wc) = refs[:13]
    (u_out, e_out, ga_out, gb_out, gc_out, gk_out, sm_out) = refs[13:20]
    (
        WA, WB, WC, WT, h1, h2, tA, gb, gbT, mean_s, inv_s, act, dpre,
        qz, kv, kvn, doz, ctxT, lse, dlt, dq, dkv,
        ra, chU, chE, finU, finE,
        ggA, ggB, ggC, ggK, r1A, r1B, r1K, r2A, r2B, r2C, r2K, f3A, f3B, f3C, f3K,
        sm, smr, smt, out, ig, wa, cosr, sinr, pos, x, send, recv, local,
    ) = refs[20:]
    ub = h2
    T, D, hs, F = d.tok, d.width, d.span, d.hidden
    nz, nc, nt, nx = d.nz, d.nc, d.nt, d.nx
    heads, B, nb, R, HR, TB = d.heads, d.blk, d.nb, d.rows, d.half, d.tile
    z, c, t = lax.axis_index("fsdp"), lax.axis_index("ctx"), lax.axis_index("tp")
    part = lax.rem(c, 2)
    other = 1 - part
    pair = c + 1 - 2 * part
    core = lax.rem(t, 2)
    xg = t // 2
    mate = t + 1 - 2 * core
    net = Net(send, recv)
    scale = HD ** (-0.5)

    def turn(value, step, size):
        return lax.rem(value + step, size)

    load_x = pltpu.make_async_copy(x_in, x, local.at[6])
    load_og = pltpu.make_async_copy(og_in, out, local.at[7])
    load_x.start()
    load_og.start()

    barrier = pltpu.get_barrier_semaphore()
    talks = []
    for rz in range(nz):
        for rc in range(nc):
            if rz or rc:
                talks.append((turn(z, rz, nz), turn(c, rc, nc), t))
    for rt in range(1, nt):
        talks.append((z, c, turn(t, rt, nt)))
    for device in talks:
        pl.semaphore_signal(barrier, inc=1, device_id=device, device_id_type=pl.DeviceIdType.MESH)
    pl.semaphore_wait(barrier, len(talks))

    half_here = pl.ds(pl.multiple_of(part * HR, HR), HR)

    def rows_of(src):
        return pl.ds(pl.multiple_of(src * R + part * HR, HR), HR)

    wa[...] = jnp.concatenate([wq_in[0], jnp.transpose(wo_in[...]), wq_in[1], wq_in[2]], 1)

    class Gather:
        def __init__(self, shard, full):
            self.moves = []
            for step in (1, -1):
                to = jnp.clip(z + step, 0, nz - 1)
                has_next = (z + 1 < nz) if step == 1 else (z > 0)
                for k in range(1, nz):
                    sent, come = z - step * (k - 1), z - step * k
                    inside = (come >= 0) if step == 1 else (come < nz)
                    has_sent = (sent >= 0) if step == 1 else (sent < nz)
                    at = rows_of(jnp.clip(sent, 0, nz - 1))
                    src = shard.at[half_here] if k == 1 else full.at[at]
                    hop = net.copy(src, full.at[at], (to, c, t))
                    got = rows_of(jnp.clip(come, 0, nz - 1))
                    side = net.copy(full.at[got], full.at[got], (z, pair, t))
                    self.moves.append((k, hop, side, inside, has_next, has_sent & has_next))

        def start(self):
            for k, hop, side, inside, has_next, sends in self.moves:
                if k == 1:
                    pl.when(sends)(hop.start)

        def pump(self, k):
            for i, (kk, hop, side, inside, has_next, sends) in enumerate(self.moves):
                if kk == k:
                    onward = self.moves[i + 1] if k + 1 < nz else None

                    @pl.when(inside)
                    def _():
                        hop.wait_recv()
                        if onward is not None:
                            pl.when(has_next)(onward[1].start)
                        side.start()

        def done(self):
            for k, hop, side, inside, has_next, sends in self.moves:
                pl.when(inside)(side.wait_recv)

        def drain(self):
            for k, hop, side, inside, has_next, sends in self.moves:
                pl.when(sends)(hop.wait_send)
                pl.when(inside)(side.wait_send)

    gather_a, gather_b, gather_c = [
        Gather(shard, full) for shard, full in ((wa, WA), (wb, WB), (wc, WC))
    ]
    gather_a.start()

    sm[...] = jnp.zeros_like(sm)
    g1, b1, g2, b2 = [one[...].reshape(1, D) for one in (gain1, shift1, gain2, shift2)]
    bf1 = bf_in[...].reshape(1, F)
    positions = pos_in[...].reshape(1, T)
    exponent = lax.broadcasted_iota(jnp.int32, (HALF, 1), 0).astype(F32) * (-2.0 / ROT)
    freqs = jnp.exp(exponent * math.log(10000.0))
    for i in range(nb):
        pos[i] = positions[:, i * B : (i + 1) * B]
        angle = pos[i].astype(F32) * freqs
        cosr[i] = jnp.cos(angle)
        sinr[i] = jnp.sin(angle)
    bq = jnp.concatenate(
        [jnp.transpose(jnp.broadcast_to(bq_in[j : j + 1, :], (128, hs)))[:, :1] for j in range(3)], 0
    )

    def norm_tile(i, carry):
        rows = tile_rows(i, TB)
        xf = x[rows, :].astype(F32)
        mean = jnp.mean(xf, -1, keepdims=True)
        cen = xf - mean
        inv = lax.rsqrt(jnp.mean(cen * cen, -1, keepdims=True) + NORM_EPS)
        normed = cen * inv
        mean_s[rows, :] = mean
        inv_s[rows, :] = inv
        h1[rows, :] = (normed * g1 + b1).astype(BF16)
        h2[rows, :] = (normed * g2 + b2).astype(BF16)
        grad = out[rows, :]
        gb[rows, :] = grad.astype(BF16)
        sm[4:5, :D] += jnp.sum(grad, 0, keepdims=True)
        return carry

    load_x.wait()
    load_og.wait()
    lax.fori_loop(0, T // TB, norm_tile, 0)
    own_rows = pl.ds(pl.multiple_of(z * R, R), R)
    WA[own_rows, :] = wa[...]
    WB[own_rows, :] = wb[...]
    WC[own_rows, :] = wc[...]
    for i in range(nb):
        gbT[i] = jnp.transpose(gb[i * B : (i + 1) * B, :])
        tA[:, i * B : (i + 1) * B] = jnp.transpose(h2[i * B : (i + 1) * B, :])

    for k in range(1, nz):
        gather_a.pump(k)
        if k == max(1, nz - 2):
            gather_b.start()
    gather_a.done()
    gather_b.pump(1)
    gather_c.start()
    WT[...] = jnp.transpose(WA[...])

    for i in range(nb):
        hidden = h1[i * B : (i + 1) * B, :]
        proj = jnp.concatenate([mm_nt(WT[:hs, :], hidden), mm_nt(WT[2 * hs :, :], hidden)], 0) + bq
        cb, sb = cosr[i], sinr[i]

        def rotated(tensor):
            lo, hi = tensor[:HALF], tensor[HALF:ROT]
            return jnp.concatenate([lo * cb - hi * sb, hi * cb + lo * sb, tensor[ROT:]], 0)

        own = c * nb + i
        for h in range(heads):
            q = rotated(proj[h * HD : (h + 1) * HD]).astype(BF16) * jnp.asarray(scale, BF16)
            qz[i, h] = jnp.concatenate([q, jnp.zeros_like(q)], 0)
            key = rotated(proj[hs + h * HD : hs + (h + 1) * HD]).astype(BF16)
            value = proj[2 * hs + h * HD : 2 * hs + (h + 1) * HD].astype(BF16)
            both = jnp.concatenate([key, value], 0)
            kv[own, h] = both
            if d.keep:
                kvn[own, h] = jnp.transpose(both)
        if i == 0 and nb > 1:
            gather_b.pump(2)

    for k in range(2 + (nb > 1), nz):
        gather_b.pump(k)
    own_blocks = pl.ds(c * nb, nb)
    kv_out = [
        net.copy(kv.at[own_blocks], kv.at[own_blocks], (z, turn(c, r, nc), t))
        for r in range(1, nc)
    ]
    gather_c.pump(1)

    for i in range(nb):
        dct = mm(WT[hs : 2 * hs, :], gbT[i]).astype(BF16)
        for h in range(heads):
            piece = dct[h * HD : (h + 1) * HD]
            doz[i, h] = jnp.concatenate([jnp.zeros_like(piece), piece], 0)

    for k in range(2, nz):
        gather_c.pump(k)
    for r, one in enumerate(kv_out, 1):

        @pl.when(c + r < nc)
        def _(one=one):
            one.start()

    gather_b.done()
    gather_c.done()

    def normed_of(rows):
        return (x[rows, :].astype(F32) - mean_s[rows, :]) * inv_s[rows, :]

    def mlp_tile(i, carry):
        rows = tile_rows(i, TB)
        pre = mm(h2[rows, :], WB[...]) + bf1
        cdf = 0.5 * (1.0 + lax.erf(pre * INV_ROOT_TWO))
        density = jnp.exp(-0.5 * pre * pre) * INV_ROOT_TWO_PI
        actb = (pre * cdf).astype(BF16)
        act[rows, :] = actb
        dp = mm(gb[rows, :], WC[...]) * (cdf + pre * density)
        sm[5:6, :F] += jnp.sum(dp, 0, keepdims=True)
        dpb = dp.astype(BF16)
        dpre[rows, :] = dpb
        out[rows, :] = mm_nt(actb, WC[...])
        dh2 = mm_nt(dpb, WB[...])
        sm[2:3, :D] += jnp.sum(dh2 * normed_of(rows), 0, keepdims=True)
        sm[3:4, :D] += jnp.sum(dh2, 0, keepdims=True)
        ig[rows, :] = dh2 * g2
        return carry

    lax.fori_loop(0, T // TB, mlp_tile, 0)

    def store_grad(gg, value, z0):
        for k in range(value.shape[0] // HR):
            gg[k % 2, z0 + k // 2] = value[k * HR : (k + 1) * HR].astype(BF16)

    class Reduce:
        def __init__(self, i, gg, r1, r2, f3, final):
            self.gg, self.r1, self.r2, self.f3 = gg, r1, r2, f3
            self.put = pltpu.make_async_copy(f3, final, local.at[i])
            self.a = [
                net.copy(gg.at[other, turn(z, r, nz)], r1.at[turn(z, r, nz)], (z, pair, t))
                for r in range(nz)
            ]
            self.b = [
                net.copy(gg.at[part, turn(z, r, nz)], r2.at[r - 1], (turn(z, r, nz), c, t))
                for r in range(1, nz)
            ]
            self.c = [net.copy(f3.at[c], f3.at[c], (z, turn(c, r, nc), t)) for r in range(1, nc)]

        def one(self):
            for one in [*self.a[1:], self.a[0]]:
                one.start()

        def two(self):
            for r in range(1, nz):
                self.a[r].wait_recv()
                zz = turn(z, r, nz)
                self.gg[part, zz] = (self.gg[part, zz].astype(F32) + self.r1[zz].astype(F32)).astype(BF16)
                self.b[r - 1].start()

        def three(self):
            self.a[0].wait_recv()
            total = self.gg[part, z].astype(F32) + self.r1[z].astype(F32)
            for r in range(1, nz):
                self.b[r - 1].wait_recv()
                total += self.r2[r - 1].astype(F32)
            self.f3[c] = total.astype(BF16)
            for one in self.c:
                one.start()

        def four(self):
            for one in self.c:
                one.wait_recv()
            self.put.start()

        def drain(self):
            for one in [*self.a, *self.b, *self.c]:
                one.wait_send()

    class ReduceFlat:
        def __init__(self, i, gg, r2, f3, final):
            self.gg, self.r2, self.f3 = gg, r2, f3
            self.put = pltpu.make_async_copy(f3, final, local.at[i])
            self.b = [
                net.copy(gg.at[turn(z, r, nz)], r2.at[r - 1], (turn(z, r, nz), c, t))
                for r in range(1, nz)
            ]
            self.c = [net.copy(f3.at[c], f3.at[c], (z, turn(c, r, nc), t)) for r in range(1, nc)]

        def one(self):
            for one in self.b:
                one.start()

        def three(self):
            total = self.gg[z].astype(F32)
            for r in range(1, nz):
                self.b[r - 1].wait_recv()
                total += self.r2[r - 1].astype(F32)
            self.f3[c] = total.astype(BF16)
            for one in self.c:
                one.start()

        def four(self):
            for one in self.c:
                one.wait_recv()
            self.put.start()

        def drain(self):
            for one in [*self.b, *self.c]:
                one.wait_send()

    redB = Reduce(0, ggB, r1B, r2B, f3B, gb_out)
    redC = ReduceFlat(1, ggC, r2C, f3C, gc_out)
    redA = Reduce(2, ggA, r1A, r2A, f3A, ga_out)
    redK = Reduce(5, ggK, r1K, r2K, f3K, gk_out)

    for z0 in range(0, nz, 2):
        store_grad(ggB, mm(tA[z0 * R : (z0 + 2) * R, :], dpre[...]), z0)
    redB.one()
    for z0 in range(0, nz, 2):
        value = None
        for i in range(nb):
            term = mm(gbT[i, z0 * R : (z0 + 2) * R, :], act[i * B : (i + 1) * B, :])
            value = term if value is None else value + term
        for k in range(2):
            ggC[z0 + k] = value[k * R : (k + 1) * R].astype(BF16)
    redC.one()

    def natural(at, h):
        return kvn[at, h] if d.keep else jnp.transpose(kv[at, h])

    def allowed_of(i, at):
        query_at = (c * nb + i) * B + lax.broadcasted_iota(jnp.int32, (1, B), 1)
        key_at = at * B + lax.broadcasted_iota(jnp.int32, (B, 1), 0)
        return (key_at <= query_at) & (key_at >= query_at - pos[i])

    def forward(i):
        here = c * nb + i
        first_key = jnp.where(here >= d.tail, d.tail, 0)
        for h in range(heads):
            qh = qz[i, h]

            def key_step(at, carry, i=i, h=h, qh=qh):
                top, total, weighted = carry
                s = jnp.where(allowed_of(i, at), mm(natural(at, h), qh), NEG_FILL)
                new_top = jnp.maximum(top, jnp.max(s, 0, keepdims=True))
                w = jnp.exp(s - new_top)
                factor = jnp.exp(top - new_top)
                total = total * factor + jnp.sum(w, 0, keepdims=True)
                weighted = weighted * factor + mm(kv[at, h, HD:], w.astype(BF16))
                return new_top, total, weighted

            top, total, weighted = lax.fori_loop(
                first_key,
                here + 1,
                key_step,
                (
                    jnp.full((1, B), NEG_FILL, F32),
                    jnp.zeros((1, B), F32),
                    jnp.zeros((HD, B), F32),
                ),
            )
            lse[i, h : h + 1, :] = top + jnp.log(total)
            ctx_h = (weighted / total).astype(BF16)
            ctxT[i, h * HD : (h + 1) * HD, :] = ctx_h
            dlt[i, h : h + 1, :] = jnp.sum(
                doz[i, h, HD:].astype(F32) * ctx_h.astype(F32), 0, keepdims=True
            )

    if d.keep:
        for i in range(1, nb):
            early = (c * nb + i >= d.tail) | (c == 0)
            pl.when(early)(lambda i=i: forward(i))
    for r, one in enumerate(kv_out, 1):

        @pl.when(c >= r)
        def _(r=r, one=one):
            one.wait_recv()

            def flip(j, carry):
                at = (c - r) * nb + j
                for h in range(heads):
                    kvn[at, h] = jnp.transpose(kv[at, h])
                return carry

            if d.keep:
                lax.fori_loop(0, nb, flip, 0)

    for i in range(nb):
        if d.keep and i:
            late = (c * nb + i < d.tail) & (c > 0)
            pl.when(late)(lambda i=i: forward(i))
        else:
            forward(i)

    chunks = 2
    CH = T // 2 // chunks

    def half_rows(which, k):
        return pl.ds(pl.multiple_of(which * (T // 2) + k * CH, CH), CH)

    class Join:
        def __init__(self, ra, ch, fin):
            self.ra, self.ch, self.fin = ra, ch, fin
            self.near, self.far, self.back = [], [], []
            for k in range(chunks):
                tile = pl.ds(k * CH, CH)
                self.near.append(net.copy(ub.at[half_rows(1 - core, k)], ra.at[tile], (z, c, mate)))
                self.far.append(
                    [
                        net.copy(ch.at[xg, tile], ch.at[xg, tile], (z, c, turn(xg, r, nx) * 2 + core))
                        for r in range(1, nx)
                    ]
                )
                self.back.append(net.copy(fin.at[core, tile], fin.at[core, tile], (z, c, mate)))

        def two(self):
            for k in range(chunks):
                self.near[k].wait_recv()
                tile = slice(k * CH, (k + 1) * CH)
                self.ch[xg, tile, :] = (
                    ub[half_rows(core, k), :].astype(F32) + self.ra[tile, :].astype(F32)
                ).astype(BF16)
                for one in self.far[k]:
                    one.start()

        def three(self):
            for k in range(chunks):
                for one in self.far[k]:
                    one.wait_recv()
                tile = slice(k * CH, (k + 1) * CH)
                total = self.ch[0, tile, :].astype(F32)
                for j in range(1, nx):
                    total += self.ch[j, tile, :].astype(F32)
                self.fin[core, tile, :] = total.astype(BF16)
                self.back[k].start()

        def four(self):
            for one in self.back:
                one.wait_recv()

        def drain(self):
            for far in self.far:
                for one in far:
                    one.wait_send()
            for one in self.back:
                one.wait_send()

    join_u = Join(ra, chU, finU)
    join_e = Join(ra, chE, finE)

    dq[...] = jnp.zeros_like(dq)

    def key_back(at, h, put):
        k_t = kv[at, h, :HD]
        k_n = natural(at, h)

        def query_step(i, carry):
            dk, dv = carry
            s = mm(k_n, qz[i, h])
            ok = allowed_of(i, at)
            prob = jnp.where(ok, jnp.exp(s - lse[i, h : h + 1, :]), 0.0)
            dp = mm(k_n, doz[i, h])
            ds = (prob * (dp - dlt[i, h : h + 1, :])).astype(BF16)
            dv = dv + mm_nt(doz[i, h, HD:], prob.astype(BF16))
            dk = dk + mm_nt(qz[i, h, :HD], ds)
            dq[i, h] += mm(k_t, ds)
            return dk, dv

        begin = jnp.maximum(at - c * nb, 0)
        end = jnp.where(at < d.tail, jnp.minimum(nb, d.tail - c * nb), nb)
        zero = jnp.zeros((HD, B), F32)
        put(lax.fori_loop(begin, end, query_step, (zero, zero)))

    dkv_base = net.used
    net.used += (nc - 1) * nb

    def dkv_copy(r, j):
        owner, slot = turn(c, nc - r, nc), dkv_base + (r - 1) * nb + j
        return pltpu.make_async_remote_copy(
            src_ref=kv.at[owner * nb + j],
            dst_ref=kv.at[c * nb + j],
            send_sem=send.at[slot],
            recv_sem=recv.at[slot],
            device_id=(z, owner, t),
            device_id_type=pl.DeviceIdType.MESH,
        )

    for r in reversed(range(1, nc)):

        @pl.when(c >= r)
        def _(r=r):
            def block(j, carry):
                for h in range(heads):

                    def put(pieces, h=h):
                        kv[(c - r) * nb + j, h, :HD] = pieces[0].astype(BF16)
                        kv[(c - r) * nb + j, h, HD:] = pieces[1].astype(BF16)

                    key_back((c - r) * nb + j, h, put)
                dkv_copy(r, j).start()
                return carry

            lax.fori_loop(0, nb, block, 0)

    for i in range(nb):
        ctx_n = jnp.transpose(ctxT[i])
        for k in range(B // TB):
            rows = slice(i * B + k * TB, i * B + (k + 1) * TB)
            ub[rows, :] = (
                out[rows, :] + mm(ctx_n[k * TB : (k + 1) * TB], WT[hs : 2 * hs, :])
            ).astype(BF16)
    for one in join_u.near:
        one.start()

    join_u.two()

    def own_block(j, carry):
        for h in range(heads):

            def put(pieces, h=h):
                dkv[j, h, :HD] = pieces[0]
                dkv[j, h, HD:] = pieces[1]

            key_back(c * nb + j, h, put)
        return carry

    lax.fori_loop(0, nb, own_block, 0)
    def unrotated(g, i):
        cb, sb = cosr[i], sinr[i]
        lo, hi = g[:HALF], g[HALF:ROT]
        return jnp.concatenate([lo * cb + hi * sb, hi * cb - lo * sb, g[ROT:]], 0)

    bias_q = jnp.zeros((hs, 1), F32)
    grad_o = None
    for i in range(nb):
        d_q = jnp.concatenate([unrotated(dq[i, h] * scale, i) for h in range(heads)], 0)
        bias_q += jnp.sum(d_q, -1, keepdims=True)
        d_q = d_q.astype(BF16)
        tA[:hs, i * B : (i + 1) * B] = d_q
        act[i * B : (i + 1) * B, : 2 * hs] = jnp.transpose(
            jnp.concatenate([d_q, jnp.zeros_like(d_q)], 0)
        )
        term = mm(ctxT[i], gb[i * B : (i + 1) * B, :])
        grad_o = term if grad_o is None else grad_o + term
    grad_q = mm(tA[:hs, :], h1[...])
    grad_a = jnp.transpose(jnp.concatenate([grad_q.astype(BF16), grad_o.astype(BF16)], 0))
    store_grad(ggA, grad_a, 0)
    redA.one()
    redB.two()
    join_u.three()

    for r in range(1, nc):

        @pl.when(c + r < nc)
        def _(r=r):
            for j in range(nb):
                dkv_copy(r, j).wait_recv()
                for h in range(heads):
                    dkv[j, h] += kv[(c + r) * nb + j, h].astype(F32)

    bias_kv = jnp.zeros((2 * hs, 1), F32)
    for i in range(nb):
        pieces = [unrotated(dkv[i, h, :HD], i) for h in range(heads)]
        pieces += [dkv[i, h, HD:] for h in range(heads)]
        d_kv = jnp.concatenate(pieces, 0)
        bias_kv += jnp.sum(d_kv, -1, keepdims=True)
        d_kv = d_kv.astype(BF16)
        tA[2 * hs : 4 * hs, i * B : (i + 1) * B] = d_kv
        act[i * B : (i + 1) * B, 2 * hs : 4 * hs] = jnp.transpose(d_kv)
    bias_t = jnp.concatenate([bias_q, bias_kv], 0)
    sm[6:7, : 3 * hs] = jnp.transpose(jnp.broadcast_to(bias_t, (3 * hs, 128)))[0:1, :]
    for one in join_u.near:
        one.wait_send()

    def e_tile(i, carry):
        rows = tile_rows(i, TB)
        dh1 = mm(act[rows, :], WT[...])
        sm[0:1, :D] += jnp.sum(dh1 * normed_of(rows), 0, keepdims=True)
        sm[1:2, :D] += jnp.sum(dh1, 0, keepdims=True)
        ub[rows, :] = (ig[rows, :] + dh1 * g1).astype(BF16)
        return carry

    join_u.four()
    for k in range(chunks):
        for q in range(CH // TB):
            for which in (1 - core, core):
                e_tile(which * (T // 2 // TB) + k * (CH // TB) + q, 0)
        join_e.near[k].start()
    grad_kv = mm(tA[2 * hs : 4 * hs, :], h1[...])
    store_grad(ggK, jnp.transpose(grad_kv.astype(BF16)), 0)
    redK.one()
    join_e.two()
    redC.three()

    rank = z * nc + c
    smr[rank] = sm[...]
    small_a = []
    for rz in range(nz):
        for rc in range(nc):
            if rz or rc:
                small_a.append(
                    net.copy(smr.at[rank], smr.at[rank], (turn(z, rz, nz), turn(c, rc, nc), t))
                )
    for one in small_a:
        one.start()
    redA.two()
    redB.three()
    redK.two()

    put_u = pltpu.make_async_copy(finU, u_out, local.at[3])
    put_u.start()
    redB.four()
    redC.four()

    for one in small_a:
        one.wait_recv()
    tot = smr[0]
    for j in range(1, nz * nc):
        tot += smr[j]
    smt[t] = tot
    small_b = [net.copy(smt.at[t], smt.at[t], (z, c, turn(t, r, nt))) for r in range(1, nt)]
    for one in small_b:
        one.start()
    redA.three()
    redK.three()
    join_e.three()
    for one in small_b:
        one.wait_recv()
    tops = smt[0, 0:4, :]
    for j in range(1, nt):
        tops += smt[j, 0:4, :]
    sm_out[...] = jnp.concatenate([tops, tot[4:8, :]], 0)
    join_e.four()

    put_e = pltpu.make_async_copy(finE, e_out, local.at[4])
    put_e.start()
    redA.four()
    redK.four()

    for one in (gather_a, gather_b, gather_c):
        one.drain()
    for r, one in enumerate(kv_out, 1):

        @pl.when(c + r < nc)
        def _(one=one):
            one.wait_send()

    for r in range(1, nc):

        @pl.when(c >= r)
        def _(r=r):
            for j in range(nb):
                dkv_copy(r, j).wait_send()

    redB.drain()
    redA.drain()
    redK.drain()
    redC.drain()
    join_u.drain()
    for one in join_e.near:
        one.wait_send()
    join_e.drain()
    for one in [*small_a, *small_b]:
        one.wait_send()
    for one in (redA.put, redB.put, redC.put, redK.put, put_u, put_e):
        one.wait()
    assert net.used == d.n_copies


def body(
    mesh,
    layer_input,
    segments,
    positions,
    ln1_gain,
    ln1_bias,
    ln2_gain,
    ln2_bias,
    w_qkv,
    b_qkv,
    w_out,
    b_out,
    w_fc1,
    b_fc1,
    w_fc2,
    b_fc2,
    out_grad,
):
    d = Dims(mesh, layer_input.shape[0], layer_input.shape[1], b_qkv.shape[1], b_fc1.shape[0])
    T, D, hs, F, B, nb = d.tok, d.width, d.span, d.hidden, d.blk, d.nb
    R, HR, nz, nc = d.rows, d.half, d.nz, d.nc
    wide_a = 4 * hs
    args = (
        layer_input,
        out_grad,
        positions,
        ln1_gain,
        ln1_bias,
        ln2_gain,
        ln2_bias,
        b_qkv,
        b_fc1,
        jnp.transpose(w_qkv, (1, 0, 2)),
        w_out,
        w_fc1,
        w_fc2.T,
    )
    vm = pltpu.VMEM
    h, W = d.heads, d.wide
    scratch = [
        vm((D, wide_a), BF16), vm((D, F), BF16), vm((D, F), BF16), vm((wide_a, D), BF16),
        vm((T, D), BF16), vm((T, D), BF16), vm((D, T), BF16), vm((T, D), BF16), vm((nb, D, B), BF16),
        vm((T, 1), F32), vm((T, 1), F32), vm((T, F), BF16), vm((T, F), BF16),
        vm((nb, h, 2 * HD, B), BF16), vm((d.nkb, h, 2 * HD, B), BF16), vm((d.nkb if d.keep else 1, h, B, 2 * HD), BF16),
        vm((nb, h, 2 * HD, B), BF16), vm((nb, hs, B), BF16),
        vm((nb, 8, B), F32), vm((nb, 8, B), F32), vm((nb, h, HD, B), F32),
        vm((nb, h, 2 * HD, B), F32),
        vm((T // 2, D), BF16),
        vm((d.nx, T // 2, D), BF16), vm((d.nx, T // 2, D), BF16),
        vm((2, T // 2, D), BF16), vm((2, T // 2, D), BF16),
    ]
    owned_shapes = [(HR, 2 * hs), (HR, F), (R, F), (HR, 2 * hs)]
    scratch += [vm((2, nz, HR, 2 * hs), BF16), vm((2, nz, HR, F), BF16)]
    scratch += [vm((nz, R, F), BF16), vm((2, nz, HR, 2 * hs), BF16)]
    scratch += [vm((nz, HR, w), BF16) for w in (2 * hs, F, 2 * hs)]
    scratch += [vm((nz - 1, *shape), BF16) for shape in owned_shapes]
    scratch += [vm((nc, *shape), BF16) for shape in owned_shapes]
    scratch += [vm((8, W), F32), vm((nz * nc, 8, W), F32), vm((d.nt, 8, W), F32)]
    scratch += [vm((T, D), F32), vm((T, D), F32), vm((R, wide_a), BF16)]
    scratch += [vm((nb, HALF, B), F32), vm((nb, HALF, B), F32), vm((nb, 1, B), jnp.int32), vm((T, D), BF16)]
    scratch += [pltpu.SemaphoreType.DMA((n,)) for n in (d.n_copies, d.n_copies, 8)]

    def kernel(*refs):
        layer_kernel(d, *refs)

    fin = jax.ShapeDtypeStruct((2, T // 2, D), BF16)
    sums = [jax.ShapeDtypeStruct((nc, *shape), BF16) for shape in owned_shapes]
    in_hbm = pl.BlockSpec(memory_space=pl.ANY)
    joined, joined_e, *owned, small = pl.pallas_call(
        kernel,
        out_shape=(fin, fin, *sums, jax.ShapeDtypeStruct((8, W), F32)),
        in_specs=[in_hbm] * 2 + [pl.BlockSpec(memory_space=vm)] * (len(args) - 2),
        out_specs=[in_hbm] * 6 + [pl.BlockSpec(memory_space=vm)],
        scratch_shapes=scratch,
        compiler_params=pltpu.CompilerParams(
            collective_id=0, has_side_effects=True, vmem_limit_bytes=VMEM_BYTES
        ),
    )(*args)

    TB = d.blk

    def tiles():
        return pl.BlockSpec((TB, D), lambda i: (i, 0))

    def whole(shape):
        return pl.BlockSpec(shape, lambda i: (0,) * len(shape))

    outs = [
        ((T, D), True), ((T, D), True), ((D,), False), ((D,), False), ((D,), False), ((D,), False),
        ((3, R, hs), False), ((3, hs), False), ((hs, R), False), ((D,), False), ((R, F), False),
        ((F,), False), ((R, F), False), ((D,), False),
    ]
    results = pl.pallas_call(
        lambda *refs: finish_kernel(d, *refs),
        grid=(T // TB,),
        out_shape=[jax.ShapeDtypeStruct(shape, F32) for shape, _ in outs],
        in_specs=[tiles(), tiles(), tiles(), tiles()]
        + [whole(o.shape) for o in owned]
        + [whole((8, W)), whole((D,)), whole((D,))],
        out_specs=[tiles() if tiled else whole(shape) for shape, tiled in outs],
        compiler_params=pltpu.CompilerParams(vmem_limit_bytes=VMEM_BYTES),
    )(
        layer_input, out_grad, joined.reshape(T, D), joined_e.reshape(T, D), *owned, small, b_out, b_fc2
    )
    results = list(results)
    results[6] = jnp.transpose(results[6], (1, 0, 2))
    results[12] = results[12].T
    return tuple(results)


def finish_kernel(d, x, og, u, e, fa, fb, fc, fk, small, bo, bf2, *outs):
    out, ig, o_g1, o_b1, o_g2, o_b2, o_qkv, o_bqkv, o_wo, o_bo, o_fc1, o_bf1, o_fc2, o_bf2 = outs
    D, hs, F, HR = d.width, d.span, d.hidden, d.half
    xf = x[...].astype(F32)
    out[...] = xf + u[...].astype(F32) + (bo[...] + bf2[...]).reshape(1, D)
    cen = xf - jnp.mean(xf, -1, keepdims=True)
    inv = lax.rsqrt(jnp.mean(cen * cen, -1, keepdims=True) + NORM_EPS)
    normed = cen * inv
    ee = e[...].astype(F32)
    ig[...] = og[...] + inv * (
        ee - jnp.mean(ee, -1, keepdims=True) - normed * jnp.mean(ee * normed, -1, keepdims=True)
    )

    def summed(slots, p):
        total = slots[p].astype(F32)
        for j in range(1, d.nc // 2):
            total += slots[2 * j + p].astype(F32)
        return total

    @pl.when(pl.program_id(0) == 0)
    def _():
        for p in range(2):
            rows = slice(p * HR, (p + 1) * HR)
            o_qkv[0, rows, :] = summed(fa, p)[:, :hs]
            half_k = summed(fk, p)
            o_qkv[1, rows, :] = half_k[:, :hs]
            o_qkv[2, rows, :] = half_k[:, hs:]
            o_fc1[rows, :] = summed(fb, p)
        total = fc[0].astype(F32)
        for j in range(1, d.nc):
            total += fc[j].astype(F32)
        o_fc2[...] = total
        whole_a = jnp.concatenate([summed(fa, 0), summed(fa, 1)], 0)
        o_wo[...] = jnp.transpose(whole_a[:, hs:])
        for k, (o, n) in enumerate(
            ((o_g1, D), (o_b1, D), (o_g2, D), (o_b2, D), (o_bo, D), (o_bf1, F))
        ):
            o[...] = small[k : k + 1, :n].reshape(n)
        o_bf2[...] = small[4:5, :D].reshape(D)
        for j in range(3):
            o_bqkv[j : j + 1, :] = small[6:7, j * hs : (j + 1) * hs]


def solution(mesh):
    in_specs = (
        P(("fsdp", "ctx"), None),
        P("fsdp"),
        P(("fsdp", "ctx")),
        P(),
        P(),
        P(),
        P(),
        P("fsdp", None, "tp"),
        P(None, "tp"),
        P("tp", "fsdp"),
        P(),
        P("fsdp", "tp"),
        P("tp"),
        P("tp", "fsdp"),
        P(),
        P(("fsdp", "ctx"), None),
    )
    out_specs = (
        P(("fsdp", "ctx"), None),
        P(("fsdp", "ctx"), None),
        P(),
        P(),
        P(),
        P(),
        P("fsdp", None, "tp"),
        P(None, "tp"),
        P("tp", "fsdp"),
        P(),
        P("fsdp", "tp"),
        P("tp"),
        P("tp", "fsdp"),
        P(),
    )

    def step(*args):
        return body(mesh, *args)

    return jax.shard_map(step, mesh=mesh, in_specs=in_specs, out_specs=out_specs, check_vma=False)
```
